32 devices in a mesh: gx: 2 (over core), gy: 4 (over y, x), gz: 4 (over z).
Axes of the slice: x: 2, y: 2, z: 4, core: 2. Of those that a mesh axis runs over, the one named last changes fastest.
Arguments:
- quant_codes: int32 [64, 128, 512], P('gx', 'gy', 'gz'), may hold values from -1073741824 to 1073741824, as said below
- error_step: float32 [1], replicated, may hold values from 4e-09 to 1.5e-08
Outputs:
- decoded: float32 [64, 128, 512], P('gx', 'gy', 'gz')
The draws below stay inside these ranges and needn't reach their ends.
Inputs may be any that keep to these rules, and one draw needn't show every extreme that they name: quant_codes are the third differences (along the three dimensions, with zeros before the grid's first cells) of a field of integers between -134217728 and 134217728.
All inputs are finite; a program needn't handle non-finite values.
Results may differ from the reference program's by a relative error of at most 0.00002.
Values sent between devices are 32-bit elements; how exact they have to be, the bound alone decides.
A program may use at most 64 MiB of HBM per device.

```python
import math
import jax
import jax.numpy as jnp

QMAX = 134217728
NX = 64
NY = 128
NZ = 512


def draw_quant_codes(key, part):
    levels_grid = jax.random.randint(jax.random.fold_in(key, 11), (NX, NY, NZ), -QMAX, QMAX + 1, dtype=jnp.int32)
    first = levels_grid - jnp.pad(levels_grid, ((1, 0), (0, 0), (0, 0)))[:-1]
    second = first - jnp.pad(first, ((0, 0), (1, 0), (0, 0)))[:, :-1]
    third = second - jnp.pad(second, ((0, 0), (0, 0), (1, 0)))[:, :, :-1]
    return third.astype(jnp.int32)


def setup_inputs(seed: int = 0) -> dict:
    streams_of = jax.random.split(jax.random.key(seed), 3)
    quant_codes = draw_quant_codes(jax.random.fold_in(streams_of[2], 71), 0)
    error_step = jnp.clip(jnp.exp(jax.random.uniform(streams_of[1], (1,), jnp.float32, math.log(3.999999886872274e-09), math.log(1.4999999464748726e-08))), 3.999999886872274e-09, 1.4999999464748726e-08)
    return {"quant_codes": quant_codes, "error_step": error_step}


def reference(quant_codes, error_step):
    prefix = jnp.cumsum(quant_codes, axis=0, dtype=jnp.int32)
    prefix = jnp.cumsum(prefix, axis=1, dtype=jnp.int32)
    prefix = jnp.cumsum(prefix, axis=2, dtype=jnp.int32)
    recon = prefix.astype(jnp.float32) * error_step[0]
    padded = jnp.pad(recon, 1)
    neighbours = padded[2:, 1:-1, 1:-1] + padded[:-2, 1:-1, 1:-1]
    neighbours = neighbours + padded[1:-1, 2:, 1:-1] + padded[1:-1, :-2, 1:-1]
    neighbours = neighbours + padded[1:-1, 1:-1, 2:] + padded[1:-1, 1:-1, :-2]
    return recon + 0.5 * (neighbours / 6.0 - recon)
```

```python
import functools

import jax
import jax.numpy as jnp
from jax import lax
from jax.experimental import pallas as pl
from jax.experimental.pallas import tpu as pltpu
from jax.sharding import PartitionSpec as P

MESH = pl.DeviceIdType.MESH
I32 = jnp.int32
F32 = jnp.float32
SUB = 8
GRANT = 16 * 2**20
UNROLL = 4


def iota(shape, dim):
    return lax.broadcasted_iota(I32, shape, dim)


def turn(x, by, dim):
    n = x.shape[dim]
    by = by % n
    if by == 0:
        return x
    if dim == 1 and n % 128 != 0:
        return jnp.concatenate([x[:, n - by :], x[:, : n - by]], 1)
    return pltpu.roll(x, by, dim)


def lane_scan(x):
    n = x.shape[1]
    tri = (iota((n, n), 0) <= iota((n, n), 1)).astype(F32)
    one, big = tri.astype(jnp.bfloat16), (tri * 256.0).astype(jnp.bfloat16)

    def times(part, m):
        return jnp.dot(part.astype(F32).astype(jnp.bfloat16), m, preferred_element_type=F32)

    low = times(x & 255, one) + times((x >> 8) & 255, big)
    high = times((x >> 16) & 255, one) + times(x >> 24, big)
    return low.astype(I32) + (high.astype(I32) << 16)


def row_scan(x):
    rows, n = x.shape
    s = iota((SUB, n), 0)
    out, carry = [], None
    for b in range(rows // SUB):
        v = x[b * SUB : (b + 1) * SUB]
        for d in (1, 2, 4):
            v = v + jnp.where(s >= d, pltpu.roll(v, d, 0), 0)
        if carry is not None:
            v = v + carry
        carry = jnp.broadcast_to(v[SUB - 1 : SUB], (SUB, n))
        out.append(v)
    return jnp.concatenate(out, 0) if len(out) > 1 else out[0]


def exchange(
    mesh_sizes, q_hbm, v_ref, eh_ref,
    q, scan, xs, xup, xdn, ys, yup, hy, ydn, lines, cup, cx, cy,
    zs, zup, ds, zdn, rx, ry, ryt, ax, hxc, by, hyc, carry,
    load_sem, xss, xrs, yss, yrs, css, crs, zss, zrs, dss, drs, ready,
):
    nx, ny, nz = mesh_sizes
    ni, nj, nk = q.shape
    nb = nj // SUB
    nl = ni * nb
    X, Y, Z = (lax.axis_index(a) for a in ("gx", "gy", "gz"))
    place = {"gx": X, "gy": Y, "gz": Z}
    size = {"gx": nx, "gy": ny, "gz": nz}
    last_x, last_y, last_z = X == nx - 1, Y == ny - 1, Z == nz - 1

    load = pltpu.make_async_copy(q_hbm, q, load_sem)
    load.start()
    barrier = pltpu.get_barrier_semaphore()

    def greet(to, axis, sem):
        pl.semaphore_signal(sem, inc=1, device_id={axis: to}, device_id_type=MESH)

    @pl.when(Z > 0)
    def _():
        greet(Z - 1, "gz", barrier)

    @pl.when(Z < nz - 1)
    def _():
        greet(Z + 1, "gz", barrier)

    for dx in range(nx):
        for dy in range(ny):
            if dx or dy:
                pl.semaphore_signal(
                    barrier, inc=1, device_id_type=MESH,
                    device_id={"gx": lax.rem(X + dx, nx), "gy": lax.rem(Y + dy, ny)},
                )

    ends = []

    def hear(d):
        @pl.when(Z + d < nz)
        def _():
            pl.semaphore_wait(ready.at[d - 2], 1)

            if d < nz - 1:
                @pl.when(Z > 0)
                def _():
                    greet(Z - 1, "gz", ready.at[d - 1])

    def up(axis, src, slots, ssem, rsem, steps=None):
        for d in steps or range(1, size[axis]):
            def copy(d=d):
                return pltpu.make_async_remote_copy(
                    src_ref=src, dst_ref=slots.at[d - 1], send_sem=ssem.at[d - 1],
                    recv_sem=rsem.at[d - 1], device_id={axis: place[axis] + d},
                    device_id_type=MESH,
                )

            here = place[axis] + d < size[axis]

            @pl.when(here)
            def _():
                copy().start()

            ends.append((here, copy))

    def up_sum(axis, src, slots, ssem, rsem, total):
        total[...] = jnp.zeros_like(total)
        for d in range(1, size[axis]):
            @pl.when(place[axis] >= d)
            def _():
                pltpu.make_async_remote_copy(
                    src_ref=src, dst_ref=slots.at[d - 1], send_sem=ssem.at[d - 1],
                    recv_sem=rsem.at[d - 1], device_id={axis: place[axis]},
                    device_id_type=MESH,
                ).wait_recv()
                total[...] += slots[d - 1]

    def down_copy(axis, src, dst, n):
        return pltpu.make_async_remote_copy(
            src_ref=src, dst_ref=dst, send_sem=dss.at[n], recv_sem=drs.at[n],
            device_id={axis: place[axis] - 1}, device_id_type=MESH,
        )

    def down(axis, src, dst, n):
        here = place[axis] > 0

        @pl.when(here)
        def _():
            down_copy(axis, src, dst, n).start()

        ends.append((here, lambda: down_copy(axis, src, dst, n)))

    def down_wait(axis, src, dst, n):
        @pl.when(place[axis] < size[axis] - 1)
        def _():
            down_copy(axis, src, dst, n).wait_recv()

        @pl.when(place[axis] == size[axis] - 1)
        def _():
            dst[...] = jnp.zeros_like(dst)

    lanes = iota((SUB, nl), 1)
    subs = iota((SUB, nl), 0)

    load.wait()
    total = q[0]
    for i in range(1, ni):
        total = total + q[i]
    xs[...] = total
    for i in range(ni):
        ys[pl.ds(i, 1), :] = jnp.sum(q[i], axis=0, keepdims=True)
        hy[pl.ds(i, 1), :] = q[i, 0:1, :]
    sk = iota((SUB, nk), 0)
    lines[...] = jnp.where(
        sk == 0, jnp.sum(total, axis=0, keepdims=True),
        jnp.where(
            sk == 1, jnp.sum(q[0], axis=0, keepdims=True),
            jnp.where(sk == 2, total[0:1], 0),
        ),
    )
    beside_z = (Z > 0).astype(I32) + (Z < nz - 1).astype(I32)
    pl.semaphore_wait(barrier, nx * ny - 1 + beside_z)
    down("gy", hy, ydn, 1)
    up("gy", ys, yup, yss, yrs)

    corners = []
    for dx in range(-1, nx):
        for dy in range(-1, ny):
            if dx > 0 and dy > 0:
                slot = cup.at[(dx - 1) * (ny - 1) + dy - 1]
            elif dx == -1 and dy > 0:
                slot = cx.at[dy - 1]
            elif dx > 0 and dy == -1:
                slot = cy.at[dx - 1]
            else:
                continue
            corners.append((dx, dy, slot, len(corners)))

    def inside(x, y):
        return (x >= 0) & (x < nx) & (y >= 0) & (y < ny)

    def corner_copy(dx, dy, slot, n):
        return pltpu.make_async_remote_copy(
            src_ref=lines, dst_ref=slot, send_sem=css.at[n], recv_sem=crs.at[n],
            device_id={"gx": X + dx, "gy": Y + dy}, device_id_type=MESH,
        )

    for c in corners:
        here = inside(X + c[0], Y + c[1])

        @pl.when(here)
        def _(c=c):
            corner_copy(*c).start()

        ends.append((here, functools.partial(corner_copy, *c)))
    up("gx", xs, xup, xss, xrs)
    down("gx", q.at[0], xdn, 0)
    if nz > 2:
        @pl.when((Z > 0) & (Z < nz - 1))
        def _():
            greet(Z - 1, "gz", ready.at[0])

    step = 8

    def scan_block(g, _):
        rows = pl.ds(g * step, step)
        part = q[rows].reshape(step * nj, nk)
        scan[rows] = lane_scan(part).reshape(step, nj, nk)
        return 0

    lax.fori_loop(0, ni // step, scan_block, 0)

    block = lax.rem(lanes, nb)

    def j_scan(w):
        for d in (1, 2, 4):
            w = w + jnp.where(subs >= d, pltpu.roll(w, d, 0), 0)
        whole = jnp.broadcast_to(w[SUB - 1 : SUB], w.shape)
        for d in range(1, nb):
            w = w + jnp.where(block >= d, turn(whole, d, 1), 0)
        return w

    def i_scan(w):
        d = nb
        while d < nl:
            w = w + jnp.where(lanes >= d, turn(w, d, 1), 0)
            d *= 2
        return w

    a0 = jnp.zeros((SUB, nl), I32)
    b0 = jnp.zeros((SUB, nl), I32)
    for i in range(ni):
        for b in range(nb):
            rows = slice(b * SUB, (b + 1) * SUB)
            here = lanes == i * nb + b
            a0 = jnp.where(here, scan[i, rows, nk - 1 : nk], a0)
            b0 = jnp.where(here, q[i, rows, 0:1], b0)
    up_sum("gx", xs, xup, xss, xrs, rx)
    down_wait("gx", q.at[0], xdn, 0)
    rxv, hxv = rx[...], xdn[...]
    lx = lane_scan(jnp.concatenate([rxv, hxv], 0))
    a2 = jnp.zeros((SUB, nl), I32)
    b2 = jnp.zeros((SUB, nl), I32)
    for b in range(2 * nb):
        rows = slice(b * SUB, (b + 1) * SUB)
        a2 = jnp.where(lanes == b, lx[rows, nk - 1 : nk], a2)
        if b < nb:
            b2 = jnp.where(lanes == b, rxv[rows, 0:1], b2)
    a0 = i_scan(j_scan(a0 + jnp.where(lanes < nb, a2, 0)))
    b0 = i_scan(j_scan(b0 + jnp.where(lanes < nb, b2, 0)))
    a2 = j_scan(a2)
    for d in range(2, nz):
        @pl.when(Z > 0)
        def _(d=d):
            hear(d)

    ax[...] = row_scan(lx[:nj])
    hxc[...] = row_scan(lx[nj:])

    up_sum("gy", ys, yup, yss, yrs, ry)
    ryt[...] = jnp.zeros_like(ryt)

    def gather_lines(wanted):
        for c in corners:
            row = 0 if c[0] > 0 and c[1] > 0 else 1 if c[1] > 0 else 2
            if (row == 0) != wanted:
                continue

            @pl.when(inside(X - c[0], Y - c[1]))
            def _(c=c, row=row):
                corner_copy(*c).wait_recv()
                ryt[...] += jnp.where(sk == row, c[2][...], 0)

    upto = (iota((ni, nl), 1) // nb) >= iota((ni, nl), 0)

    def along(column, extra):
        return jnp.sum(jnp.where(upto, column, 0), axis=0, keepdims=True) + extra

    gather_lines(True)
    ds[...] = b0 + along(ry[:, 0:1], ryt[0:1, 0:1])
    down("gz", ds, zdn, 2)
    down_wait("gy", hy, ydn, 1)
    gather_lines(False)
    ryv, rytv = ry[...], ryt[...]
    ly = lane_scan(jnp.concatenate([ryv, ydn[...], rytv], 0))
    lyl, lyh, lyt = ly[:ni], ly[ni : 2 * ni], ly[2 * ni :]
    lyht = lyt[2:3]
    end = slice(nk - 1, nk)
    y_low = along(lyl[:, end], lyt[0:1, end])
    y_high = along(lyh[:, end], lyht[0:1, end])
    zs[0:SUB] = a0 + y_low
    zs[SUB : 2 * SUB] = a2 + jnp.where(lanes < nb, lyt[0:1, end], lyt[1:2, end])
    zs[2 * SUB :] = jnp.where(subs == 0, y_low, jnp.where(subs == 1, y_high, 0))
    up("gz", zs, zup, zss, zrs, [1])

    rows_i = iota((ni, nk), 0)
    by[...] = row_scan(lyl + jnp.where(rows_i == 0, lyt[0:1], 0))
    hyc[...] = row_scan(lyh + jnp.where(rows_i == 0, lyht[0:1], 0))
    jrow = iota((nj, nk), 0)
    klane = iota((nj, nk), 1)
    plane = ax[...]

    def field(i, before):
        inner = before + row_scan(scan[i])
        return inner, inner + plane + by[pl.ds(i, 1), :]

    def stencil(i, low, mid, high):
        down_j = jnp.where(jrow == 0, by[pl.ds(i, 1), :], turn(mid, 1, 0))
        edge_j = jnp.where(last_y, 0, mid + hyc[pl.ds(i, 1), :])
        up_j = jnp.where(jrow == nj - 1, edge_j, turn(mid, nj - 1, 0))
        down_k = jnp.where(klane == 0, 0, turn(mid, 1, 1))
        edge_k = jnp.where(last_z, 0, mid)
        up_k = jnp.where(klane == nk - 1, edge_k, turn(mid, nk - 1, 1))
        v_ref[i] = 6 * mid + (low + high) + (down_j + up_j) + (down_k + up_k)

    def sweep(i, state):
        low, mid, before = state
        inner, high = field(i + 1, before)
        stencil(i, low, mid, high)
        return mid, high, inner

    inner, mid = field(0, jnp.zeros((nj, nk), I32))
    state = (plane + lyt[0:1], mid, inner)
    many = (ni - 1) // UNROLL

    def sweeps(g, state):
        for u in range(UNROLL):
            state = sweep(g * UNROLL + u, state)
        return state

    state = lax.fori_loop(0, many, sweeps, state)
    for i in range(many * UNROLL, ni - 1):
        state = sweep(i, state)
    low, mid, _ = state
    stencil(ni - 1, low, mid, jnp.where(last_x, 0, mid + hxc[...] + lyt[1:2]))

    for d in range(2, nz):
        @pl.when(Z == 0)
        def _(d=d):
            hear(d)

        up("gz", zs, zup, zss, zrs, [d])

    up_sum("gz", zs, zup, zss, zrs, carry)
    down_wait("gz", ds, zdn, 2)
    D, xe = carry[0:SUB], carry[SUB : 2 * SUB]
    y_low, y_high = carry[2 * SUB : 2 * SUB + 1], carry[2 * SUB + 1 : 2 * SUB + 2]
    down_i = jnp.where(lanes < nb, xe, turn(D, nb, 1))
    edge_i = jnp.where(last_x, 0, D + turn(xe, nl - 2 * nb, 1))
    up_i = jnp.where(lanes >= nl - nb, edge_i, turn(D, nl - nb, 1))
    t = pltpu.roll(D, 1, 0)
    down_j = jnp.where(subs == 0, jnp.where(block == 0, y_low, turn(t, 1, 1)), t)
    t = pltpu.roll(D, SUB - 1, 0)
    edge_j = jnp.where(last_y, 0, D + y_high)
    up_j = jnp.where(
        subs == SUB - 1, jnp.where(block == nb - 1, edge_j, turn(t, nl - 1, 1)), t
    )
    eh_ref[0:SUB] = 8 * D + (down_i + up_i) + (down_j + up_j)
    eh_ref[SUB : 2 * SUB] = jnp.where(last_z, -D, zdn[...])

    for here, copy in ends:
        @pl.when(here)
        def _():
            copy().wait_send()


def finish(step_ref, v_ref, eh_ref, out_hbm, out, sems):
    ni, nj, nk = out.shape
    nb = nj // SUB
    scale = step_ref[0] * (1.0 / 12.0)
    at_end = iota((SUB, nk), 1) == nk - 1
    E, EH = eh_ref[0:SUB], eh_ref[0:SUB] + eh_ref[SUB : 2 * SUB]
    pieces = sems.shape[0]
    depth = ni // pieces
    copies = []
    for p in range(pieces):
        for i in range(p * depth, (p + 1) * depth):
            for b in range(nb):
                v = i * nb + b
                rows = slice(b * SUB, (b + 1) * SUB)
                carry = jnp.where(at_end, EH[:, v : v + 1], E[:, v : v + 1])
                out[i, rows, :] = (v_ref[i, rows, :] + carry).astype(F32) * scale
        part = pl.ds(p * depth, depth)
        copy = pltpu.make_async_copy(out.at[part], out_hbm.at[part], sems.at[p])
        copy.start()
        copies.append(copy)
    for copy in copies:
        copy.wait()


def solution(mesh):
    sizes = tuple(mesh.shape[a] for a in ("gx", "gy", "gz"))
    nx, ny, nz = sizes

    def on_device(quant_codes, error_step):
        ni, nj, nk = quant_codes.shape
        nl = ni * nj // SUB
        vm = lambda *shape: pltpu.VMEM(shape, I32)
        dma = lambda n: pltpu.SemaphoreType.DMA((n,))
        scratch = [
            vm(ni, nj, nk), vm(ni, nj, nk),
            vm(nj, nk), vm(nx - 1, nj, nk), vm(nj, nk),
            vm(ni, nk), vm(ny - 1, ni, nk), vm(ni, nk), vm(ni, nk),
            vm(SUB, nk), vm((nx - 1) * (ny - 1), SUB, nk),
            vm(ny - 1, SUB, nk), vm(nx - 1, SUB, nk),
            vm(3 * SUB, nl), vm(nz - 1, 3 * SUB, nl), vm(SUB, nl), vm(SUB, nl),
            vm(nj, nk), vm(ni, nk), vm(SUB, nk),
            vm(nj, nk), vm(nj, nk), vm(ni, nk), vm(ni, nk),
            vm(3 * SUB, nl),
        ]
        semaphores = [
            pltpu.SemaphoreType.DMA,
            dma(nx - 1), dma(nx - 1), dma(ny - 1), dma(ny - 1),
            dma(nx * ny - 1 + nx * ny), dma(nx * ny - 1 + nx * ny), dma(nz - 1), dma(nz - 1),
            dma(3), dma(3),
            pltpu.SemaphoreType.REGULAR((max(nz - 2, 1),)),
        ]

        def scoped(*refs):
            def body(*sems):
                exchange(sizes, *refs, *sems)

            pl.run_scoped(body, *semaphores)

        any_space = pl.BlockSpec(memory_space=pl.ANY)
        hbm = pl.BlockSpec(memory_space=pltpu.HBM)
        vmem = pl.BlockSpec(memory_space=pltpu.VMEM)
        v, eh = pl.pallas_call(
            scoped,
            out_shape=(
                jax.ShapeDtypeStruct((ni, nj, nk), I32),
                jax.ShapeDtypeStruct((2 * SUB, nl), I32),
            ),
            in_specs=[hbm],
            out_specs=(vmem, vmem),
            scratch_shapes=scratch,
            compiler_params=pltpu.CompilerParams(
                collective_id=0, has_side_effects=True, vmem_limit_bytes=GRANT
            ),
            name="exchange",
        )(pltpu.with_memory_space_constraint(quant_codes, pltpu.HBM))
        return pl.pallas_call(
            finish,
            out_shape=jax.ShapeDtypeStruct((ni, nj, nk), F32),
            in_specs=[pl.BlockSpec(memory_space=pltpu.SMEM), vmem, vmem],
            out_specs=any_space,
            scratch_shapes=[pltpu.VMEM((ni, nj, nk), F32), dma(4)],
            compiler_params=pltpu.CompilerParams(vmem_limit_bytes=16 * 2**20),
            name="finish",
        )(error_step, v, eh)

    return jax.shard_map(
        on_device, mesh=mesh, in_specs=(P("gx", "gy", "gz"), P()),
        out_specs=P("gx", "gy", "gz"), check_vma=False,
    )
```

```python
import functools

import jax
import jax.numpy as jnp
from jax import lax
from jax.experimental import pallas as pl
from jax.experimental.pallas import tpu as pltpu
from jax.sharding import PartitionSpec as P

MESH = pl.DeviceIdType.MESH
I32 = jnp.int32
F32 = jnp.float32
SUB = 8
GRANT = 16 * 2**20
UNROLL = 4
DEEP = 16


def iota(shape, dim):
    return lax.broadcasted_iota(I32, shape, dim)


def turn(x, by, dim):
    n = x.shape[dim]
    by = by % n
    if by == 0:
        return x
    if dim == 1 and n % 128 != 0:
        return jnp.concatenate([x[:, n - by :], x[:, : n - by]], 1)
    return pltpu.roll(x, by, dim)


def lane_scan(x):
    n = x.shape[1]
    tri = (iota((n, n), 0) <= iota((n, n), 1)).astype(F32)
    one, big = tri.astype(jnp.bfloat16), (tri * 256.0).astype(jnp.bfloat16)

    def times(part, m):
        return jnp.dot(part.astype(F32).astype(jnp.bfloat16), m, preferred_element_type=F32)

    low = times(x & 255, one) + times((x >> 8) & 255, big)
    high = times((x >> 16) & 255, one) + times(x >> 24, big)
    return low.astype(I32) + (high.astype(I32) << 16)


def row_scan(x):
    rows, n = x.shape
    s = iota((SUB, n), 0)
    out, carry = [], None
    for b in range(rows // SUB):
        v = x[b * SUB : (b + 1) * SUB]
        for d in (1, 2, 4):
            v = v + jnp.where(s >= d, pltpu.roll(v, d, 0), 0)
        if carry is not None:
            v = v + carry
        carry = jnp.broadcast_to(v[SUB - 1 : SUB], (SUB, n))
        out.append(v)
    return jnp.concatenate(out, 0) if len(out) > 1 else out[0]


def exchange(
    mesh_sizes, q_hbm, v_ref, eh_ref,
    q, scan, xs, xup, xdn, ys, yup, hy, ydn, pk, pkin, dgin,
    zs, zup, ds, zdn, ax, hxc, by, hyc,
    load_sem, xss, xrs, yss, yrs, pss, prs, gss, grs, zss, zrs, dss, drs, ready,
):
    nx, ny, nz = mesh_sizes
    ni, nj, nk = q.shape
    nb = nj // SUB
    nl = ni * nb
    X, Y, Z = (lax.axis_index(a) for a in ("gx", "gy", "gz"))
    place = {"gx": X, "gy": Y, "gz": Z}
    size = {"gx": nx, "gy": ny, "gz": nz}
    last_x, last_y, last_z = X == nx - 1, Y == ny - 1, Z == nz - 1
    plane_to, level_to = messages(nx, ny)

    load = pltpu.make_async_copy(q_hbm, q, load_sem)
    load.start()
    barrier = pltpu.get_barrier_semaphore()

    def greet(to, sem):
        pl.semaphore_signal(sem, inc=1, device_id=to, device_id_type=MESH)

    def inside(x, y, z=0):
        ok = (x >= 0) & (x < nx) & (y >= 0) & (y < ny)
        return ok if isinstance(z, int) else ok & (z >= 0) & (z < nz)

    for dx in range(nx):
        for dy in range(ny):
            if dx or dy:
                greet({"gx": lax.rem(X + dx, nx), "gy": lax.rem(Y + dy, ny)}, barrier)
    first_y = Y == 0
    for d in (-2, -1, 1):
        @pl.when((Z + d >= 0) & (Z + d < nz) & (first_y if d == -2 else True))
        def _(d=d):
            greet({"gz": Z + d}, barrier)

    for dx, dy in level_to:
        @pl.when(inside(X - dx, Y - dy, Z + 1))
        def _(dx=dx, dy=dy):
            greet({"gx": X - dx, "gy": Y - dy, "gz": Z + 1}, barrier)

    near = sum(((Z + d >= 0) & (Z + d < nz)).astype(I32) for d in (-1, 1))
    near = near + (first_y & (Z + 2 < nz)).astype(I32)
    above = jnp.where(Z > 0, (nx - X) * (ny - 1 - Y), 0)
    awaited = nx * ny - 1 + near + above

    def clear(here, slot):
        @pl.when(here)
        def _():
            slot[...] = jnp.zeros(slot.shape, I32)

    for n, (dx, dy) in enumerate(plane_to):
        clear(jnp.logical_not(inside(X - dx, Y - dy)), pkin.at[n])
    for n, (dx, dy) in enumerate(level_to):
        clear(jnp.logical_not(inside(X - dx, Y - dy, Z + 1)), dgin.at[n])
    for axis, slots, beyond in (("gx", xup, xdn), ("gy", yup, ydn), ("gz", zup, zdn)):
        for d in range(1, size[axis]):
            clear(place[axis] < d, slots.at[d - 1])
        clear(place[axis] == size[axis] - 1, beyond)

    ends = []

    def send(here, copy):
        @pl.when(here)
        def _():
            copy().start()

    def up_copy(axis, src, slots, ssem, rsem, d):
        return pltpu.make_async_remote_copy(
            src_ref=src, dst_ref=slots.at[d - 1], send_sem=ssem.at[d - 1],
            recv_sem=rsem.at[d - 1], device_id={axis: place[axis] + d},
            device_id_type=MESH,
        )

    def ups(axis, *refs):
        return [
            (place[axis] + d < size[axis], functools.partial(up_copy, axis, *refs, d))
            for d in range(size[axis] - 1, 0, -1)
        ]

    def up_wait(axis, *refs):
        for d in range(1, size[axis]):
            @pl.when(place[axis] >= d)
            def _(d=d):
                up_copy(axis, *refs, d).wait_recv()

    def down_copy(axis, src, dst, n):
        return pltpu.make_async_remote_copy(
            src_ref=src, dst_ref=dst, send_sem=dss.at[n], recv_sem=drs.at[n],
            device_id={axis: place[axis] - 1}, device_id_type=MESH,
        )

    def downs(axis, src, dst, n):
        return [(place[axis] > 0, functools.partial(down_copy, axis, src, dst, n))]

    def down_wait(axis, src, dst, n):
        @pl.when(place[axis] < size[axis] - 1)
        def _():
            down_copy(axis, src, dst, n).wait_recv()

    def plane_copy(n):
        return pltpu.make_async_remote_copy(
            src_ref=pk, dst_ref=pkin.at[n], send_sem=pss.at[n], recv_sem=prs.at[n],
            device_id={"gx": X + plane_to[n][0], "gy": Y + plane_to[n][1]},
            device_id_type=MESH,
        )

    def level_copy(n):
        return pltpu.make_async_remote_copy(
            src_ref=pk.at[0:SUB], dst_ref=dgin.at[n], send_sem=gss.at[n],
            recv_sem=grs.at[n], device_id_type=MESH,
            device_id={"gx": X + level_to[n][0], "gy": Y + level_to[n][1], "gz": Z - 1},
        )

    lanes = iota((SUB, nl), 1)
    subs = iota((SUB, nl), 0)
    sk = iota((SUB, nk), 0)
    block = lax.rem(lanes, nb)
    end = slice(nk - 1, nk)
    upto = (iota((ni, nl), 1) // nb) >= iota((ni, nl), 0)

    def along(column):
        return jnp.sum(jnp.where(upto, column, 0), axis=0, keepdims=True)

    def j_scan(w):
        for d in (1, 2, 4):
            w = w + jnp.where(subs >= d, pltpu.roll(w, d, 0), 0)
        whole = jnp.broadcast_to(w[SUB - 1 : SUB], w.shape)
        for d in range(1, nb):
            w = w + jnp.where(block >= d, turn(whole, d, 1), 0)
        return w

    def i_scan(w):
        d = nb
        while d < nl:
            w = w + jnp.where(lanes >= d, turn(w, d, 1), 0)
            d *= 2
        return w

    load.wait()
    total = q[0]
    for i in range(1, ni):
        total = total + q[i]
    xs[...] = total
    for i in range(ni):
        ys[pl.ds(i, 1), :] = jnp.sum(q[i], axis=0, keepdims=True)
        hy[pl.ds(i, 1), :] = q[i, 0:1, :]
    lines = jnp.where(
        sk == 0, jnp.sum(total, axis=0, keepdims=True),
        jnp.where(
            sk == 1, jnp.sum(q[0], axis=0, keepdims=True),
            jnp.where(sk == 2, total[0:1], 0),
        ),
    )
    ysv = ys[...]
    small = lane_scan(jnp.concatenate([ysv, hy[...], lines], 0))[:, end]
    ends_of = jnp.broadcast_to(small[2 * ni :], (SUB, nl))
    row = [
        along(small[:ni]), ends_of[0:1], along(ysv[:, 0:1]),
        jnp.broadcast_to(lines[0:1, 0:1], (1, nl)), along(small[ni : 2 * ni]),
        ends_of[2:3], ends_of[1:2],
    ]
    rows = jnp.zeros((SUB, nl), I32)
    for r, value in enumerate(row):
        rows = jnp.where(subs == r, value, rows)
    pk[0:SUB] = rows
    pk[SUB:] = lines

    outgoing = [
        (inside(X + dx, Y + dy), functools.partial(plane_copy, n))
        for n, (dx, dy) in enumerate(plane_to)
    ] + [
        (inside(X + dx, Y + dy, Z - 1), functools.partial(level_copy, n))
        for n, (dx, dy) in enumerate(level_to)
    ]
    outgoing += ups("gx", xs, xup, xss, xrs) + downs("gx", q.at[0], xdn, 0)
    outgoing += downs("gy", hy, ydn, 1) + ups("gy", ys, yup, yss, yrs)
    ends.extend(outgoing)
    relays = [
        (base, (Z > 0) & (Z + base < nz) & (first_y == (base == 2)))
        for base in (1, 2) if nz > base + 1
    ]

    def burst():
        pl.semaphore_wait(barrier, awaited)
        for here, copy in outgoing:
            send(here, copy)
        for base, here in relays:
            @pl.when(here)
            def _(base=base):
                greet({"gz": Z - 1}, ready.at[base - 1])

    @pl.when(jnp.logical_not(first_y))
    def _():
        burst()

    deep = min(DEEP, ni)

    def scan_block(g, _):
        part = q[pl.ds(g * deep, deep)].reshape(deep * nj, nk)
        scan[pl.ds(g * deep, deep)] = lane_scan(part).reshape(deep, nj, nk)
        return 0

    lax.fori_loop(0, ni // deep, scan_block, 0)

    a0 = jnp.zeros((SUB, nl), I32)
    b0 = jnp.zeros((SUB, nl), I32)
    for i in range(ni):
        for b in range(nb):
            rows_b = slice(b * SUB, (b + 1) * SUB)
            here = lanes == i * nb + b
            a0 = jnp.where(here, scan[i, rows_b, end], a0)
            b0 = jnp.where(here, q[i, rows_b, 0:1], b0)
    a0 = i_scan(j_scan(a0))
    b0 = i_scan(j_scan(b0))
    ds[...] = b0

    @pl.when(first_y)
    def _():
        burst()

    [(below, down_ds)] = downs("gz", ds, zdn, 2)
    ends.append((below, down_ds))
    send(below & (X == 0), down_ds)

    def hear(d, also):
        @pl.when((Z + d < nz) & also & (True if d > 2 else jnp.logical_not(first_y)))
        def _():
            pl.semaphore_wait(ready.at[d - 2], 1)

            if d < nz - 1:
                @pl.when(Z > 0)
                def _():
                    greet({"gz": Z - 1}, ready.at[d - 1])

    for d in range(2, nz):
        hear(d, Z > 0)

    up_wait("gx", xs, xup, xss, xrs)
    down_wait("gx", q.at[0], xdn, 0)
    rxv = xup[0]
    for d in range(1, nx - 1):
        rxv = rxv + xup[d]
    lx = lane_scan(jnp.concatenate([rxv, xdn[...]], 0))
    a2 = jnp.zeros((SUB, nl), I32)
    b2 = jnp.zeros((SUB, nl), I32)
    for b in range(2 * nb):
        rows_b = slice(b * SUB, (b + 1) * SUB)
        a2 = jnp.where(lanes == b, lx[rows_b, end], a2)
        if b < nb:
            b2 = jnp.where(lanes == b, rxv[rows_b, 0:1], b2)
    a2 = j_scan(a2)
    b2 = j_scan(b2)
    a0 = a0 + i_scan(jnp.where(lanes < nb, a2, 0))

    @pl.when(X > 0)
    def _():
        ds[...] += i_scan(jnp.where(lanes < nb, b2, 0))

    send(below & (X > 0), down_ds)
    ax[...] = row_scan(lx[:nj])
    hxc[...] = row_scan(lx[nj:])

    for n, (dx, dy) in enumerate(plane_to):
        @pl.when(inside(X - dx, Y - dy))
        def _(n=n):
            plane_copy(n).wait_recv()

    def gather(wanted, slots):
        found = [slots(n) for n, m in enumerate(plane_to) if wanted(*m)]
        return functools.reduce(jnp.add, found) if found else jnp.zeros((SUB, nk), I32)

    kinds = (
        (lambda dx, dy: dx == 0 and dy > 0, 0), (lambda dx, dy: dx > 0 and dy > 0, 1),
        (lambda dx, dy: dx == 0 and dy < 0, 4), (lambda dx, dy: dx > 0 and dy < 0, 5),
        (lambda dx, dy: dx < 0, 6),
    )
    low, corner, high, high_corner, before = (
        gather(wanted, lambda n: pkin[n, 0:SUB])[r : r + 1] for wanted, r in kinds
    )
    y_low, y_high = low + corner, high + high_corner
    zs[0:SUB] = a0 + y_low
    zs[SUB : 2 * SUB] = a2 + jnp.where(lanes < nb, corner, before)
    zs[2 * SUB :] = jnp.where(subs == 0, y_low, jnp.where(subs == 1, y_high, 0))
    z_refs = (zs, zup, zss, zrs)
    higher = ups("gz", *z_refs)
    ends.extend(higher)
    for here, copy in higher:
        send(here & (Z > 0), copy)
    for d, (here, copy) in enumerate(reversed(higher), 1):
        if d > 1:
            hear(d, Z == 0)
        send(here & (Z == 0), copy)

    up_wait("gy", ys, yup, yss, yrs)
    down_wait("gy", hy, ydn, 1)
    ryv = yup[0]
    for d in range(1, ny - 1):
        ryv = ryv + yup[d]
    tail = lambda n: pkin[n, SUB:]
    rytv = jnp.where(
        sk == 0, gather(kinds[1][0], tail),
        jnp.where(
            sk == 1, gather(kinds[4][0], tail),
            jnp.where(sk == 2, gather(kinds[3][0], tail), 0),
        ),
    )
    ly = lane_scan(jnp.concatenate([ryv, ydn[...], rytv], 0))
    lyl, lyh, lyt = ly[:ni], ly[ni : 2 * ni], ly[2 * ni :]
    rows_i = iota((ni, nk), 0)
    by[...] = row_scan(lyl + jnp.where(rows_i == 0, lyt[0:1], 0))
    hyc[...] = row_scan(lyh + jnp.where(rows_i == 0, lyt[2:3], 0))
    jrow = iota((nj, nk), 0)
    klane = iota((nj, nk), 1)
    plane = ax[...]

    def field(i, before):
        inner = before + row_scan(scan[i])
        return inner, inner + plane + by[pl.ds(i, 1), :]

    def stencil(i, low, mid, high):
        down_j = jnp.where(jrow == 0, by[pl.ds(i, 1), :], turn(mid, 1, 0))
        edge_j = jnp.where(last_y, 0, mid + hyc[pl.ds(i, 1), :])
        up_j = jnp.where(jrow == nj - 1, edge_j, turn(mid, nj - 1, 0))
        down_k = jnp.where(klane == 0, 0, turn(mid, 1, 1))
        edge_k = jnp.where(last_z, 0, mid)
        up_k = jnp.where(klane == nk - 1, edge_k, turn(mid, nk - 1, 1))
        v_ref[i] = 6 * mid + (low + high) + (down_j + up_j) + (down_k + up_k)

    def sweep(i, state):
        low, mid, before = state
        inner, high = field(i + 1, before)
        stencil(i, low, mid, high)
        return mid, high, inner

    inner, mid = field(0, jnp.zeros((nj, nk), I32))
    state = (plane + lyt[0:1], mid, inner)
    many = (ni - 1) // UNROLL

    def sweeps(g, state):
        for u in range(UNROLL):
            state = sweep(g * UNROLL + u, state)
        return state

    state = lax.fori_loop(0, many, sweeps, state)
    for i in range(many * UNROLL, ni - 1):
        state = sweep(i, state)
    low, mid, _ = state
    stencil(ni - 1, low, mid, jnp.where(last_x, 0, mid + hxc[...] + lyt[1:2]))

    for n, (dx, dy) in enumerate(level_to):
        @pl.when(inside(X - dx, Y - dy, Z + 1))
        def _(n=n):
            level_copy(n).wait_recv()

    down_wait("gz", ds, zdn, 2)
    up_wait("gz", *z_refs)
    beyond = zdn[...]
    for n, (dx, dy) in enumerate(level_to):
        r = 2 if dx == 0 else 3
        beyond = beyond + dgin[n, r : r + 1, :]
    carry = zup[0]
    for d in range(1, nz - 1):
        carry = carry + zup[d]
    D, xe = carry[0:SUB], carry[SUB : 2 * SUB]
    y_low, y_high = carry[2 * SUB : 2 * SUB + 1], carry[2 * SUB + 1 : 2 * SUB + 2]
    down_i = jnp.where(lanes < nb, xe, turn(D, nb, 1))
    edge_i = jnp.where(last_x, 0, D + turn(xe, nl - 2 * nb, 1))
    up_i = jnp.where(lanes >= nl - nb, edge_i, turn(D, nl - nb, 1))
    t = pltpu.roll(D, 1, 0)
    down_j = jnp.where(subs == 0, jnp.where(block == 0, y_low, turn(t, 1, 1)), t)
    t = pltpu.roll(D, SUB - 1, 0)
    edge_j = jnp.where(last_y, 0, D + y_high)
    up_j = jnp.where(
        subs == SUB - 1, jnp.where(block == nb - 1, edge_j, turn(t, nl - 1, 1)), t
    )
    eh_ref[0:SUB] = 8 * D + (down_i + up_i) + (down_j + up_j)
    eh_ref[SUB : 2 * SUB] = jnp.where(last_z, -D, beyond)

    for here, copy in ends:
        @pl.when(here)
        def _():
            copy().wait_send()


def messages(nx, ny):
    plane = [
        (dx, dy) for dy in range(ny - 1, 0, -1) for dx in range(-1, nx)
    ] + [(dx, -1) for dx in range(nx)]
    level = [(dx, dy) for dy in range(ny - 1, 0, -1) for dx in range(nx)]
    return plane, level


def finish(step_ref, v_ref, eh_ref, out_hbm, out, sems):
    ni, nj, nk = out.shape
    nb = nj // SUB
    scale = step_ref[0] * (1.0 / 12.0)
    at_end = iota((SUB, nk), 1) == nk - 1
    E, EH = eh_ref[0:SUB], eh_ref[0:SUB] + eh_ref[SUB : 2 * SUB]
    pieces = sems.shape[0]
    depth = ni // pieces
    copies = []
    for p in range(pieces):
        for i in range(p * depth, (p + 1) * depth):
            for b in range(nb):
                v = i * nb + b
                rows = slice(b * SUB, (b + 1) * SUB)
                carry = jnp.where(at_end, EH[:, v : v + 1], E[:, v : v + 1])
                out[i, rows, :] = (v_ref[i, rows, :] + carry).astype(F32) * scale
        part = pl.ds(p * depth, depth)
        copy = pltpu.make_async_copy(out.at[part], out_hbm.at[part], sems.at[p])
        copy.start()
        copies.append(copy)
    for copy in copies:
        copy.wait()


def solution(mesh):
    sizes = tuple(mesh.shape[a] for a in ("gx", "gy", "gz"))
    nx, ny, nz = sizes

    def on_device(quant_codes, error_step):
        ni, nj, nk = quant_codes.shape
        nl = ni * nj // SUB
        vm = lambda *shape: pltpu.VMEM(shape, I32)
        dma = lambda n: pltpu.SemaphoreType.DMA((n,))
        plane_to, level_to = messages(nx, ny)
        np_, ng = len(plane_to), len(level_to)
        scratch = [
            vm(ni, nj, nk), vm(ni, nj, nk),
            vm(nj, nk), vm(nx - 1, nj, nk), vm(nj, nk),
            vm(ni, nk), vm(ny - 1, ni, nk), vm(ni, nk), vm(ni, nk),
            vm(2 * SUB, nl), vm(np_, 2 * SUB, nl), vm(ng, SUB, nl),
            vm(3 * SUB, nl), vm(nz - 1, 3 * SUB, nl), vm(SUB, nl), vm(SUB, nl),
            vm(nj, nk), vm(nj, nk), vm(ni, nk), vm(ni, nk),
        ]
        semaphores = [
            pltpu.SemaphoreType.DMA,
            dma(nx - 1), dma(nx - 1), dma(ny - 1), dma(ny - 1),
            dma(np_), dma(np_), dma(ng), dma(ng), dma(nz - 1), dma(nz - 1),
            dma(3), dma(3),
            pltpu.SemaphoreType.REGULAR((max(nz - 2, 1),)),
        ]

        def scoped(*refs):
            def body(*sems):
                exchange(sizes, *refs, *sems)

            pl.run_scoped(body, *semaphores)

        any_space = pl.BlockSpec(memory_space=pl.ANY)
        hbm = pl.BlockSpec(memory_space=pltpu.HBM)
        vmem = pl.BlockSpec(memory_space=pltpu.VMEM)
        v, eh = pl.pallas_call(
            scoped,
            out_shape=(
                jax.ShapeDtypeStruct((ni, nj, nk), I32),
                jax.ShapeDtypeStruct((2 * SUB, nl), I32),
            ),
            in_specs=[hbm],
            out_specs=(vmem, vmem),
            scratch_shapes=scratch,
            compiler_params=pltpu.CompilerParams(
                collective_id=0, has_side_effects=True, vmem_limit_bytes=GRANT
            ),
            name="exchange",
        )(pltpu.with_memory_space_constraint(quant_codes, pltpu.HBM))
        return pl.pallas_call(
            finish,
            out_shape=jax.ShapeDtypeStruct((ni, nj, nk), F32),
            in_specs=[pl.BlockSpec(memory_space=pltpu.SMEM), vmem, vmem],
            out_specs=any_space,
            scratch_shapes=[pltpu.VMEM((ni, nj, nk), F32), dma(4)],
            compiler_params=pltpu.CompilerParams(vmem_limit_bytes=16 * 2**20),
            name="finish",
        )(error_step, v, eh)

    return jax.shard_map(
        on_device, mesh=mesh, in_specs=(P("gx", "gy", "gz"), P()),
        out_specs=P("gx", "gy", "gz"), check_vma=False,
    )
```

```python
import functools

import jax
import jax.numpy as jnp
from jax import lax
from jax.experimental import pallas as pl
from jax.experimental.pallas import tpu as pltpu
from jax.sharding import PartitionSpec as P

MESH = pl.DeviceIdType.MESH
I32 = jnp.int32
F32 = jnp.float32
SUB = 8
GRANT = 16 * 2**20
UNROLL = 4
DEEP = 16
TURNS = 8


def iota(shape, dim):
    return lax.broadcasted_iota(I32, shape, dim)


def turn(x, by, dim):
    n = x.shape[dim]
    by = by % n
    if by == 0:
        return x
    if dim == 1 and n % 128 != 0:
        return jnp.concatenate([x[:, n - by :], x[:, : n - by]], 1)
    return pltpu.roll(x, by, dim)


def lane_scan(x):
    n = x.shape[1]
    tri = (iota((n, n), 0) <= iota((n, n), 1)).astype(F32)
    one, big = tri.astype(jnp.bfloat16), (tri * 256.0).astype(jnp.bfloat16)

    def times(part, m):
        return jnp.dot(part.astype(F32).astype(jnp.bfloat16), m, preferred_element_type=F32)

    low = times(x & 255, one) + times((x >> 8) & 255, big)
    high = times((x >> 16) & 255, one) + times(x >> 24, big)
    return low.astype(I32) + (high.astype(I32) << 16)


def row_scan(x):
    rows, n = x.shape
    s = iota((SUB, n), 0)
    out, carry = [], None
    for b in range(rows // SUB):
        v = x[b * SUB : (b + 1) * SUB]
        for d in (1, 2, 4):
            v = v + jnp.where(s >= d, pltpu.roll(v, d, 0), 0)
        if carry is not None:
            v = v + carry
        carry = jnp.broadcast_to(v[SUB - 1 : SUB], (SUB, n))
        out.append(v)
    return jnp.concatenate(out, 0) if len(out) > 1 else out[0]


def exchange(
    mesh_sizes, q_hbm, v_ref, eh_ref,
    q, scan, xs, xup, xdn, ys, yup, hy, ydn, pk, pkin, px, pxin, dgin,
    zs, zup, ds, zdn, ax, hxc, by, hyc, tails,
    load_sem, xss, xrs, yss, yrs, pss, prs, ass, ars, gss, grs, zss, zrs, dss, drs, ready,
):
    nx, ny, nz = mesh_sizes
    ni, nj, nk = q.shape
    nb = nj // SUB
    nl = ni * nb
    X, Y, Z = (lax.axis_index(a) for a in ("gx", "gy", "gz"))
    place = {"gx": X, "gy": Y, "gz": Z}
    size = {"gx": nx, "gy": ny, "gz": nz}
    last_x, last_y, last_z = X == nx - 1, Y == ny - 1, Z == nz - 1
    plane_to, level_to = messages(nx, ny)
    beside = [-1, *range(1, nx)]

    load = pltpu.make_async_copy(q_hbm, q, load_sem)
    load.start()
    barrier = pltpu.get_barrier_semaphore()

    def greet(to, sem):
        pl.semaphore_signal(sem, inc=1, device_id=to, device_id_type=MESH)

    def inside(x, y, z=0):
        ok = (x >= 0) & (x < nx) & (y >= 0) & (y < ny)
        return ok if isinstance(z, int) else ok & (z >= 0) & (z < nz)

    for dx in range(nx):
        for dy in range(ny):
            if dx or dy:
                greet({"gx": lax.rem(X + dx, nx), "gy": lax.rem(Y + dy, ny)}, barrier)
    first_y = Y == 0
    for d in (-2, -1, 1):
        @pl.when((Z + d >= 0) & (Z + d < nz) & (first_y if d == -2 else True))
        def _(d=d):
            greet({"gz": Z + d}, barrier)

    for dx, dy in level_to:
        @pl.when(inside(X - dx, Y - dy, Z + 1))
        def _(dx=dx, dy=dy):
            greet({"gx": X - dx, "gy": Y - dy, "gz": Z + 1}, barrier)

    near = sum(((Z + d >= 0) & (Z + d < nz)).astype(I32) for d in (-1, 1))
    near = near + (first_y & (Z + 2 < nz)).astype(I32)
    above = jnp.where(Z > 0, (nx - X) * (ny - Y) - 1, 0)
    awaited = nx * ny - 1 + near + above

    def clear(here, slot):
        @pl.when(here)
        def _():
            slot[...] = jnp.zeros(slot.shape, I32)

    for n, (dx, dy) in enumerate(plane_to):
        clear(jnp.logical_not(inside(X - dx, Y - dy)), pkin.at[n])
    for n, dx in enumerate(beside):
        clear(jnp.logical_not(inside(X - dx, Y)), pxin.at[n])
    for n, (dx, dy) in enumerate(level_to):
        clear(jnp.logical_not(inside(X - dx, Y - dy, Z + 1)), dgin.at[n])
    for axis, slots, beyond in (("gx", xup, xdn), ("gy", yup, ydn), ("gz", zup, zdn)):
        for d in range(1, size[axis]):
            clear(place[axis] < d, slots.at[d - 1])
        clear(place[axis] == size[axis] - 1, beyond)

    def send(here, copy):
        @pl.when(here)
        def _():
            copy().start()

    def finish_sends(started):
        for here, copy in started:
            @pl.when(here)
            def _(copy=copy):
                copy().wait_send()

    def up_copy(axis, src, slots, ssem, rsem, d):
        return pltpu.make_async_remote_copy(
            src_ref=src, dst_ref=slots.at[d - 1], send_sem=ssem.at[d - 1],
            recv_sem=rsem.at[d - 1], device_id={axis: place[axis] + d},
            device_id_type=MESH,
        )

    def ups(axis, *refs):
        return [
            (place[axis] + d < size[axis], functools.partial(up_copy, axis, *refs, d))
            for d in range(size[axis] - 1, 0, -1)
        ]

    def up_wait(axis, *refs):
        for d in range(1, size[axis]):
            @pl.when(place[axis] >= d)
            def _(d=d):
                up_copy(axis, *refs, d).wait_recv()

    def down_copy(axis, src, dst, n):
        return pltpu.make_async_remote_copy(
            src_ref=src, dst_ref=dst, send_sem=dss.at[n], recv_sem=drs.at[n],
            device_id={axis: place[axis] - 1}, device_id_type=MESH,
        )

    def downs(axis, src, dst, n):
        return [(place[axis] > 0, functools.partial(down_copy, axis, src, dst, n))]

    def down_wait(axis, src, dst, n):
        @pl.when(place[axis] < size[axis] - 1)
        def _():
            down_copy(axis, src, dst, n).wait_recv()

    def plane_copy(n):
        return pltpu.make_async_remote_copy(
            src_ref=pk if plane_to[n][0] else pk.at[0:SUB],
            dst_ref=pkin.at[n] if plane_to[n][0] else pkin.at[n, 0:SUB],
            send_sem=pss.at[n], recv_sem=prs.at[n],
            device_id={"gx": X + plane_to[n][0], "gy": Y + plane_to[n][1]},
            device_id_type=MESH,
        )

    def beside_copy(n):
        return pltpu.make_async_remote_copy(
            src_ref=px, dst_ref=pxin.at[n], send_sem=ass.at[n], recv_sem=ars.at[n],
            device_id={"gx": X + beside[n]}, device_id_type=MESH,
        )

    def level_copy(n):
        return pltpu.make_async_remote_copy(
            src_ref=pk.at[0:SUB] if level_to[n][1] else px.at[SUB : 2 * SUB],
            dst_ref=dgin.at[n], send_sem=gss.at[n],
            recv_sem=grs.at[n], device_id_type=MESH,
            device_id={"gx": X + level_to[n][0], "gy": Y + level_to[n][1], "gz": Z - 1},
        )

    lanes = iota((SUB, nl), 1)
    subs = iota((SUB, nl), 0)
    sk = iota((SUB, nk), 0)
    block = lax.rem(lanes, nb)
    half = nl // 2
    moved = (subs > 1) & (subs < 4) & (lax.rem(lanes, 2 * nb) >= nb)
    end = slice(nk - 1, nk)
    upto = (iota((ni, nl), 1) // nb) >= iota((ni, nl), 0)

    def along(column):
        return jnp.sum(jnp.where(upto, column, 0), axis=0, keepdims=True)

    def j_scan(w):
        for d in (1, 2, 4):
            w = w + jnp.where(subs >= d, pltpu.roll(w, d, 0), 0)
        whole = jnp.broadcast_to(w[SUB - 1 : SUB], w.shape)
        for d in range(1, nb):
            w = w + jnp.where(block >= d, turn(whole, d, 1), 0)
        return w

    def packed(column):
        w = jnp.zeros((SUB, nl), I32)
        for b in range(nb):
            w = jnp.where(block == b, column[b * SUB : (b + 1) * SUB], w)
        return w

    def i_scan(w):
        d = nb
        while d < nl:
            w = w + jnp.where(lanes >= d, turn(w, d, 1), 0)
            d *= 2
        return w

    load.wait()
    total = q[0]
    for i in range(1, ni):
        total = total + q[i]
    xs[...] = total
    for i in range(ni):
        ys[pl.ds(i, 1), :] = jnp.sum(q[i], axis=0, keepdims=True)
        hy[pl.ds(i, 1), :] = q[i, 0:1, :]
    lines = jnp.where(
        sk == 0, jnp.sum(total, axis=0, keepdims=True),
        jnp.where(
            sk == 1, jnp.sum(q[0], axis=0, keepdims=True),
            jnp.where(sk == 2, total[0:1], 0),
        ),
    )
    ysv = ys[...]
    small = lane_scan(jnp.concatenate([ysv, hy[...], lines, total, q[0]], 0))[:, end]
    ends_of = jnp.broadcast_to(small[2 * ni : 2 * ni + SUB], (SUB, nl))
    row = [
        along(small[:ni]), ends_of[0:1], along(ysv[:, 0:1]),
        jnp.broadcast_to(lines[0:1, 0:1], (1, nl)), along(small[ni : 2 * ni]),
        ends_of[2:3], ends_of[1:2],
    ]
    rows = jnp.zeros((SUB, nl), I32)
    for r, value in enumerate(row):
        rows = jnp.where(subs == r, value, rows)
    pk[0:SUB] = rows
    pk[SUB:] = lines

    outgoing = [
        (inside(X + dx, Y + dy), functools.partial(plane_copy, n))
        for n, (dx, dy) in enumerate(plane_to)
    ] + [
        (inside(X + dx, Y + dy, Z - 1), functools.partial(level_copy, n))
        for n, (dx, dy) in enumerate(level_to)
    ]
    outgoing += [
        (inside(X + dx, Y), functools.partial(beside_copy, n)) for n, dx in enumerate(beside)
    ]
    outgoing += ups("gx", xs, xup, xss, xrs) + downs("gx", q.at[0], xdn, 0)
    outgoing += downs("gy", hy, ydn, 1) + ups("gy", ys, yup, yss, yrs)
    relays = [
        (base, (Z > 0) & (Z + base < nz) & (first_y == (base == 2)))
        for base in (1, 2) if nz > base + 1
    ]

    def burst(before=()):
        pl.semaphore_wait(barrier, awaited)
        for here, copy in [*before, *outgoing]:
            send(here, copy)
        for base, here in relays:
            @pl.when(here)
            def _(base=base):
                greet({"gz": Z - 1}, ready.at[base - 1])

    first = 2 * ni + SUB
    px[0:SUB] = j_scan(packed(small[first : first + nj]))
    px[SUB : 2 * SUB] = j_scan(packed(total[:, 0:1]))
    px[2 * SUB :] = j_scan(packed(small[first + nj :]))
    @pl.when(jnp.logical_not(first_y))
    def _():
        burst()

    deep = min(DEEP, ni)

    def scan_block(g, _):
        part = q[pl.ds(g * deep, deep)].reshape(deep * nj, nk)
        scan[pl.ds(g * deep, deep)] = lane_scan(part).reshape(deep, nj, nk)
        return 0

    lax.fori_loop(0, ni // deep, scan_block, 0)

    def columns(source, column):
        w = jnp.zeros((SUB, nl), I32)
        for i in range(ni):
            for b in range(nb):
                part = source[i, b * SUB : (b + 1) * SUB, column]
                w = jnp.where(lanes == i * nb + b, part, w)
        return i_scan(j_scan(w))

    ds[...] = columns(q, slice(0, 1))
    [(below, down_ds)] = downs("gz", ds, zdn, 2)

    @pl.when(first_y)
    def _():
        burst([(below, down_ds)])

    send(below & jnp.logical_not(first_y), down_ds)
    a0 = columns(scan, end)

    def hear(d, also):
        @pl.when((Z + d < nz) & also & (True if d > 2 else jnp.logical_not(first_y)))
        def _():
            pl.semaphore_wait(ready.at[d - 2], 1)

            if d < nz - 1:
                @pl.when(Z > 0)
                def _():
                    greet({"gz": Z - 1}, ready.at[d - 1])

    for d in range(2, nz):
        hear(d, Z > 0)

    for n, dx in enumerate(beside):
        @pl.when(inside(X - dx, Y))
        def _(n=n):
            beside_copy(n).wait_recv()

    xa = pxin[1, 0:SUB]
    for n in range(2, nx):
        xa = xa + pxin[n, 0:SUB]
    a0 = a0 + xa
    xd = pxin[0, 2 * SUB :]
    up_wait("gx", xs, xup, xss, xrs)
    down_wait("gx", q.at[0], xdn, 0)
    rxv = xup[0]
    for d in range(1, nx - 1):
        rxv = rxv + xup[d]
    lx = lane_scan(jnp.concatenate([rxv, xdn[...]], 0))
    ax[...] = row_scan(lx[:nj])
    hxc[...] = row_scan(lx[nj:])

    def sweep_all():
        jrow = iota((nj, nk), 0)
        klane = iota((nj, nk), 1)
        plane = ax[...]

        def field(i, before):
            inner = before + row_scan(scan[i])
            return inner, inner + plane + by[pl.ds(i, 1), :]

        def stencil(i, low, mid, high):
            down_j = jnp.where(jrow == 0, by[pl.ds(i, 1), :], turn(mid, 1, 0))
            edge_j = jnp.where(last_y, 0, mid)
            up_j = jnp.where(jrow == nj - 1, edge_j, turn(mid, nj - 1, 0))
            down_k = jnp.where(klane == 0, 0, turn(mid, 1, 1))
            edge_k = jnp.where(last_z, 0, mid)
            up_k = jnp.where(klane == nk - 1, edge_k, turn(mid, nk - 1, 1))
            v_ref[i] = 6 * mid + (low + high) + (down_j + up_j) + (down_k + up_k)

        def sweep(i, state):
            low, mid, before = state
            inner, high = field(i + 1, before)
            stencil(i, low, mid, high)
            return mid, high, inner

        inner, mid = field(0, jnp.zeros((nj, nk), I32))
        state = (plane + tails[0:1], mid, inner)
        many = (ni - 1) // UNROLL

        def sweeps(g, state):
            for u in range(UNROLL):
                state = sweep(g * UNROLL + u, state)
            return state

        state = lax.fori_loop(0, many, sweeps, state)
        for i in range(many * UNROLL, ni - 1):
            state = sweep(i, state)
        low, mid, _ = state
        stencil(ni - 1, low, mid, jnp.where(last_x, 0, mid + hxc[...] + tails[1:2]))

    @pl.when(first_y)
    def _():
        tails[...] = jnp.zeros_like(tails)
        by[...] = jnp.zeros_like(by)
        sweep_all()

    for n, (dx, dy) in enumerate(plane_to):
        @pl.when(inside(X - dx, Y - dy))
        def _(n=n):
            plane_copy(n).wait_recv()

    def gather(wanted, slots):
        found = [slots(n) for n, m in enumerate(plane_to) if wanted(*m)]
        return functools.reduce(jnp.add, found) if found else jnp.zeros((SUB, nk), I32)

    kinds = (
        (lambda dx, dy: dx == 0 and dy > 0, 0), (lambda dx, dy: dx > 0 and dy > 0, 1),
        (lambda dx, dy: dx == 0 and dy < 0, 4), (lambda dx, dy: dx > 0 and dy < 0, 5),
        (lambda dx, dy: dx < 0, 6),
    )
    low, corner, high, high_corner, before = (
        gather(wanted, lambda n: pkin[n, 0:SUB])[r : r + 1] for wanted, r in kinds
    )
    y_low, y_high = low + corner, high + high_corner
    front, back = xa + corner, xd + before
    zs[0:SUB] = a0 + y_low
    zs[SUB:] = jnp.where(
        subs == 0, y_low,
        jnp.where(
            subs == 1, y_high,
            jnp.where(
                lanes < half, jnp.where(moved, pltpu.roll(front, 2, 0), front),
                jnp.where(moved, pltpu.roll(back, 2, 0), back),
            ),
        ),
    )
    z_refs = (zs, zup, zss, zrs)
    higher = ups("gz", *z_refs)
    for d in range(2, nz):
        hear(d, Z == 0)
    for here, copy in higher:
        send(here, copy)

    up_wait("gy", ys, yup, yss, yrs)
    down_wait("gy", hy, ydn, 1)
    ryv = yup[0]
    for d in range(1, ny - 1):
        ryv = ryv + yup[d]
    tail = lambda n: pkin[n, SUB:]
    rytv = jnp.where(
        sk == 0, gather(kinds[1][0], tail),
        jnp.where(
            sk == 1, gather(kinds[4][0], tail),
            jnp.where(sk == 2, gather(kinds[3][0], tail), 0),
        ),
    )
    ly = lane_scan(jnp.concatenate([ryv, ydn[...], rytv], 0))
    lyl, lyh, lyt = ly[:ni], ly[ni : 2 * ni], ly[2 * ni :]
    rows_i = iota((ni, nk), 0)
    hyc[...] = row_scan(lyh + jnp.where(rows_i == 0, lyt[2:3], 0))

    @pl.when(jnp.logical_not(first_y))
    def _():
        tails[...] = lyt
        by[...] = row_scan(lyl + jnp.where(rows_i == 0, lyt[0:1], 0))
        sweep_all()

    for i in range(ni):
        beyond_j = jnp.where(sk == SUB - 1, hyc[pl.ds(i, 1), :], 0)
        v_ref[i, nj - SUB : nj, :] += jnp.where(last_y, 0, beyond_j)

    finish_sends([*outgoing, (below, down_ds)])
    for n, (dx, dy) in enumerate(level_to):
        @pl.when(inside(X - dx, Y - dy, Z + 1))
        def _(n=n):
            level_copy(n).wait_recv()

    down_wait("gz", ds, zdn, 2)
    up_wait("gz", *z_refs)
    beyond = zdn[...]
    for n, (dx, dy) in enumerate(level_to):
        r = 2 if dx == 0 else 3
        beyond = beyond + (dgin[n, r : r + 1, :] if dy else dgin[n])
    carry = zup[0]
    for d in range(1, nz - 1):
        carry = carry + zup[d]
    D, edges = carry[0:SUB], carry[SUB:]
    y_low = jnp.broadcast_to(edges[0:1], D.shape)
    y_high = jnp.where(last_y, 0, jnp.broadcast_to(edges[1:2], D.shape))
    lifted = pltpu.roll(edges, SUB - 2, 0)
    prior, after = pltpu.roll(D, 1, 0), pltpu.roll(D, SUB - 1, 0)

    def finals(by):
        at = lax.rem(lanes + (nl - by), nl)
        moved_to = lambda w, d: turn(w, d + by, 1)
        here = moved_to(D, 0)
        front = jnp.where(subs < 2, moved_to(lifted, nl - nb), moved_to(edges, 0))
        back = jnp.where(subs < 2, moved_to(lifted, 0), moved_to(edges, nb))
        down_i = jnp.where(at < nb, front, moved_to(D, nb))
        edge_i = jnp.where(last_x, 0, here + back)
        up_i = jnp.where(at >= nl - nb, edge_i, moved_to(D, nl - nb))
        edge_j = jnp.where(block == 0, moved_to(y_low, 0), moved_to(prior, 1))
        down_j = jnp.where(subs == 0, edge_j, moved_to(prior, 0))
        edge_j = jnp.where(last_y, 0, here + moved_to(y_high, 0))
        edge_j = jnp.where(block == nb - 1, edge_j, moved_to(after, nl - 1))
        up_j = jnp.where(subs == SUB - 1, edge_j, moved_to(after, 0))
        E = 8 * here + (down_i + up_i) + (down_j + up_j)
        return E, E + jnp.where(last_z, -here, moved_to(beyond, 0))

    E, EH = finals(0)
    E_half, EH_half = finals(half)
    eh_ref[0:SUB] = jnp.where(lanes < half, E, EH_half)
    eh_ref[SUB : 2 * SUB] = jnp.where(lanes < half, E_half, EH)

    finish_sends(higher)


def messages(nx, ny):
    plane = [(dx, -1) for dx in range(nx)] + [
        (dx, dy) for dy in range(ny - 1, 0, -1) for dx in range(-1, nx)
    ]
    level = [(dx, dy) for dy in range(ny - 1, -1, -1) for dx in range(nx) if dx or dy]
    return plane, level


def finish(step_ref, v_ref, eh_ref, out_hbm, out, sems):
    ni, nj, nk = out.shape
    nb = nj // SUB
    scale = step_ref[0] * (1.0 / 12.0)
    half = ni * nb // 2
    base = jnp.where(iota((SUB, nk), 1) == nk - 1, half, 0)
    halves = eh_ref[0:SUB], eh_ref[SUB : 2 * SUB]
    steps = sems.shape[0] // 2
    depth = ni // 2 // steps
    turned = [[turn(w, half * 2 - c, 1) for c in range(TURNS)] for w in halves]
    copies = []
    for p in range(steps):
        for i in range(p * depth, (p + 1) * depth):
            for b in range(nb):
                v = i * nb + b
                c = v % TURNS
                rows = slice(b * SUB, (b + 1) * SUB)
                for at, source in ((i, turned[0][c]), (i + ni // 2, turned[1][c])):
                    carry = jnp.take_along_axis(
                        source, base + (v - c), 1, mode="promise_in_bounds"
                    )
                    out[at, rows, :] = (v_ref[at, rows, :] + carry).astype(F32) * scale
        for h in range(2):
            part = pl.ds(h * (ni // 2) + p * depth, depth)
            copy = pltpu.make_async_copy(out.at[part], out_hbm.at[part], sems.at[2 * p + h])
            copy.start()
            copies.append(copy)
    for copy in copies:
        copy.wait()


def solution(mesh):
    sizes = tuple(mesh.shape[a] for a in ("gx", "gy", "gz"))
    nx, ny, nz = sizes

    def on_device(quant_codes, error_step):
        ni, nj, nk = quant_codes.shape
        nl = ni * nj // SUB
        vm = lambda *shape: pltpu.VMEM(shape, I32)
        dma = lambda n: pltpu.SemaphoreType.DMA((n,))
        plane_to, level_to = messages(nx, ny)
        np_, ng = len(plane_to), len(level_to)
        scratch = [
            vm(ni, nj, nk), vm(ni, nj, nk),
            vm(nj, nk), vm(nx - 1, nj, nk), vm(nj, nk),
            vm(ni, nk), vm(ny - 1, ni, nk), vm(ni, nk), vm(ni, nk),
            vm(2 * SUB, nl), vm(np_, 2 * SUB, nl), vm(3 * SUB, nl), vm(nx, 3 * SUB, nl),
            vm(ng, SUB, nl),
            vm(2 * SUB, nl), vm(nz - 1, 2 * SUB, nl), vm(SUB, nl), vm(SUB, nl),
            vm(nj, nk), vm(nj, nk), vm(ni, nk), vm(ni, nk), vm(SUB, nk),
        ]
        semaphores = [
            pltpu.SemaphoreType.DMA,
            dma(nx - 1), dma(nx - 1), dma(ny - 1), dma(ny - 1),
            dma(np_), dma(np_), dma(nx), dma(nx), dma(ng), dma(ng), dma(nz - 1), dma(nz - 1),
            dma(3), dma(3),
            pltpu.SemaphoreType.REGULAR((max(nz - 2, 1),)),
        ]

        def scoped(*refs):
            def body(*sems):
                exchange(sizes, *refs, *sems)

            pl.run_scoped(body, *semaphores)

        any_space = pl.BlockSpec(memory_space=pl.ANY)
        hbm = pl.BlockSpec(memory_space=pltpu.HBM)
        vmem = pl.BlockSpec(memory_space=pltpu.VMEM)
        v, eh = pl.pallas_call(
            scoped,
            out_shape=(
                jax.ShapeDtypeStruct((ni, nj, nk), I32),
                jax.ShapeDtypeStruct((2 * SUB, nl), I32),
            ),
            in_specs=[hbm],
            out_specs=(vmem, vmem),
            scratch_shapes=scratch,
            compiler_params=pltpu.CompilerParams(
                collective_id=0, has_side_effects=True, vmem_limit_bytes=GRANT
            ),
            name="exchange",
        )(pltpu.with_memory_space_constraint(quant_codes, pltpu.HBM))
        return pl.pallas_call(
            finish,
            out_shape=jax.ShapeDtypeStruct((ni, nj, nk), F32),
            in_specs=[pl.BlockSpec(memory_space=pltpu.SMEM), vmem, vmem],
            out_specs=any_space,
            scratch_shapes=[pltpu.VMEM((ni, nj, nk), F32), dma(8)],
            compiler_params=pltpu.CompilerParams(vmem_limit_bytes=16 * 2**20),
            name="finish",
        )(error_step, v, eh)

    return jax.shard_map(
        on_device, mesh=mesh, in_specs=(P("gx", "gy", "gz"), P()),
        out_specs=P("gx", "gy", "gz"), check_vma=False,
    )
```

```python
import functools

import jax
import jax.numpy as jnp
from jax import lax
from jax.experimental import pallas as pl
from jax.experimental.pallas import tpu as pltpu
from jax.sharding import PartitionSpec as P

MESH = pl.DeviceIdType.MESH
I32 = jnp.int32
F32 = jnp.float32
SUB = 8
GRANT = 16 * 2**20
UNROLL = 4
DEEP = 16
TURNS = 8


def iota(shape, dim):
    return lax.broadcasted_iota(I32, shape, dim)


def turn(x, by, dim):
    n = x.shape[dim]
    by = by % n
    if by == 0:
        return x
    if dim == 1 and n % 128 != 0:
        return jnp.concatenate([x[:, n - by :], x[:, : n - by]], 1)
    return pltpu.roll(x, by, dim)


def lane_scan(x):
    n = x.shape[1]
    tri = (iota((n, n), 0) <= iota((n, n), 1)).astype(F32)
    one, big = tri.astype(jnp.bfloat16), (tri * 256.0).astype(jnp.bfloat16)

    def times(part, m):
        return jnp.dot(part.astype(F32).astype(jnp.bfloat16), m, preferred_element_type=F32)

    low = times(x & 255, one) + times((x >> 8) & 255, big)
    high = times((x >> 16) & 255, one) + times(x >> 24, big)
    return low.astype(I32) + (high.astype(I32) << 16)


def row_scan(x):
    rows, n = x.shape
    s = iota((SUB, n), 0)
    out, carry = [], None
    for b in range(rows // SUB):
        v = x[b * SUB : (b + 1) * SUB]
        for d in (1, 2, 4):
            v = v + jnp.where(s >= d, pltpu.roll(v, d, 0), 0)
        if carry is not None:
            v = v + carry
        carry = jnp.broadcast_to(v[SUB - 1 : SUB], (SUB, n))
        out.append(v)
    return jnp.concatenate(out, 0) if len(out) > 1 else out[0]


def exchange(
    mesh_sizes, q_hbm, v_ref, eh_ref,
    q, scan, xs, xup, xdn, ys, yup, hy, ydn, pk, pkin, px, pxin, dgin,
    zs, zup, zr, zrin, ds, zdn, ax, hxc, by, hyc, tails,
    load_sem, xss, xrs, yss, yrs, pss, prs, ass, ars, gss, grs, zss, zrs, rss, rrs, dss, drs, ready,
):
    nx, ny, nz = mesh_sizes
    ni, nj, nk = q.shape
    nb = nj // SUB
    nl = ni * nb
    X, Y, Z = (lax.axis_index(a) for a in ("gx", "gy", "gz"))
    place = {"gx": X, "gy": Y, "gz": Z}
    size = {"gx": nx, "gy": ny, "gz": nz}
    last_x, last_y, last_z = X == nx - 1, Y == ny - 1, Z == nz - 1
    plane_to, level_to = messages(nx, ny)
    beside = [-1, *range(1, nx)]

    load = pltpu.make_async_copy(q_hbm, q, load_sem)
    load.start()
    barrier = pltpu.get_barrier_semaphore()

    def greet(to, sem):
        pl.semaphore_signal(sem, inc=1, device_id=to, device_id_type=MESH)

    def inside(x, y, z=0):
        ok = (x >= 0) & (x < nx) & (y >= 0) & (y < ny)
        return ok if isinstance(z, int) else ok & (z >= 0) & (z < nz)

    for dx in range(nx):
        for dy in range(ny):
            if dx or dy:
                greet({"gx": lax.rem(X + dx, nx), "gy": lax.rem(Y + dy, ny)}, barrier)
    first_y = Y == 0
    for d in (-2, -1, 1):
        @pl.when((Z + d >= 0) & (Z + d < nz) & (first_y if d == -2 else True))
        def _(d=d):
            greet({"gz": Z + d}, barrier)

    for dx, dy in level_to:
        @pl.when(inside(X - dx, Y - dy, Z + 1))
        def _(dx=dx, dy=dy):
            greet({"gx": X - dx, "gy": Y - dy, "gz": Z + 1}, barrier)

    near = sum(((Z + d >= 0) & (Z + d < nz)).astype(I32) for d in (-1, 1))
    near = near + (first_y & (Z + 2 < nz)).astype(I32)
    above = jnp.where(Z > 0, (nx - X) * (ny - Y) - 1, 0)
    awaited = nx * ny - 1 + near + above

    def clear(here, slot):
        @pl.when(here)
        def _():
            slot[...] = jnp.zeros(slot.shape, I32)

    for n, (dx, dy) in enumerate(plane_to):
        clear(jnp.logical_not(inside(X - dx, Y - dy)), pkin.at[n])
    for n, dx in enumerate(beside):
        clear(jnp.logical_not(inside(X - dx, Y)), pxin.at[n])
    for n, (dx, dy) in enumerate(level_to):
        clear(jnp.logical_not(inside(X - dx, Y - dy, Z + 1)), dgin.at[n])
    for axis, slots, beyond in (("gx", xup, xdn), ("gy", yup, ydn), ("gz", zup, zdn), ("gz", zrin, None)):
        for d in range(1, size[axis]):
            clear(place[axis] < d, slots.at[d - 1])
        if beyond is not None:
            clear(place[axis] == size[axis] - 1, beyond)

    def send(here, copy):
        @pl.when(here)
        def _():
            copy().start()

    def finish_sends(started):
        for here, copy in started:
            @pl.when(here)
            def _(copy=copy):
                copy().wait_send()

    def up_copy(axis, src, slots, ssem, rsem, d):
        return pltpu.make_async_remote_copy(
            src_ref=src, dst_ref=slots.at[d - 1], send_sem=ssem.at[d - 1],
            recv_sem=rsem.at[d - 1], device_id={axis: place[axis] + d},
            device_id_type=MESH,
        )

    def ups(axis, *refs):
        return [
            (place[axis] + d < size[axis], functools.partial(up_copy, axis, *refs, d))
            for d in range(size[axis] - 1, 0, -1)
        ]

    def up_wait(axis, *refs):
        for d in range(1, size[axis]):
            @pl.when(place[axis] >= d)
            def _(d=d):
                up_copy(axis, *refs, d).wait_recv()

    def down_copy(axis, src, dst, n):
        return pltpu.make_async_remote_copy(
            src_ref=src, dst_ref=dst, send_sem=dss.at[n], recv_sem=drs.at[n],
            device_id={axis: place[axis] - 1}, device_id_type=MESH,
        )

    def downs(axis, src, dst, n):
        return [(place[axis] > 0, functools.partial(down_copy, axis, src, dst, n))]

    def down_wait(axis, src, dst, n):
        @pl.when(place[axis] < size[axis] - 1)
        def _():
            down_copy(axis, src, dst, n).wait_recv()

    def plane_copy(n):
        return pltpu.make_async_remote_copy(
            src_ref=pk if plane_to[n][0] else pk.at[0:SUB],
            dst_ref=pkin.at[n] if plane_to[n][0] else pkin.at[n, 0:SUB],
            send_sem=pss.at[n], recv_sem=prs.at[n],
            device_id={"gx": X + plane_to[n][0], "gy": Y + plane_to[n][1]},
            device_id_type=MESH,
        )

    def beside_copy(n):
        return pltpu.make_async_remote_copy(
            src_ref=px, dst_ref=pxin.at[n], send_sem=ass.at[n], recv_sem=ars.at[n],
            device_id={"gx": X + beside[n]}, device_id_type=MESH,
        )

    def level_copy(n):
        return pltpu.make_async_remote_copy(
            src_ref=pk.at[0:SUB] if level_to[n][1] else px.at[SUB : 2 * SUB],
            dst_ref=dgin.at[n], send_sem=gss.at[n],
            recv_sem=grs.at[n], device_id_type=MESH,
            device_id={"gx": X + level_to[n][0], "gy": Y + level_to[n][1], "gz": Z - 1},
        )

    lanes = iota((SUB, nl), 1)
    subs = iota((SUB, nl), 0)
    sk = iota((SUB, nk), 0)
    block = lax.rem(lanes, nb)
    half = nl // 2
    starts = (0, nj, 2 * nj, 2 * nj + ni, 2 * (nj + ni))
    lane = iota((1, nl), 1)

    def within(k):
        return (lane >= starts[k]) & (lane < starts[k + 1])

    def in_order(column, k):
        n = column.shape[0]
        at = iota((n, nl), 1) - starts[k]
        reached = (at >= iota((n, nl), 0)) & (at < n)
        return jnp.sum(jnp.where(reached, column, 0), axis=0, keepdims=True)
    end = slice(nk - 1, nk)
    upto = (iota((ni, nl), 1) // nb) >= iota((ni, nl), 0)

    def along(column):
        return jnp.sum(jnp.where(upto, column, 0), axis=0, keepdims=True)

    def j_scan(w):
        for d in (1, 2, 4):
            w = w + jnp.where(subs >= d, pltpu.roll(w, d, 0), 0)
        whole = jnp.broadcast_to(w[SUB - 1 : SUB], w.shape)
        for d in range(1, nb):
            w = w + jnp.where(block >= d, turn(whole, d, 1), 0)
        return w

    def stacked(values):
        w = jnp.zeros((SUB, nl), I32)
        for r, value in enumerate(values):
            w = jnp.where(subs == r, value, w)
        return w

    def packed(column):
        w = jnp.zeros((SUB, nl), I32)
        for b in range(nb):
            w = jnp.where(block == b, column[b * SUB : (b + 1) * SUB], w)
        return w

    def i_scan(w):
        d = nb
        while d < nl:
            w = w + jnp.where(lanes >= d, turn(w, d, 1), 0)
            d *= 2
        return w

    load.wait()
    total = q[0]
    for i in range(1, ni):
        total = total + q[i]
    xs[...] = total
    for i in range(ni):
        ys[pl.ds(i, 1), :] = jnp.sum(q[i], axis=0, keepdims=True)
        hy[pl.ds(i, 1), :] = q[i, 0:1, :]
    lines = jnp.where(
        sk == 0, jnp.sum(total, axis=0, keepdims=True),
        jnp.where(
            sk == 1, jnp.sum(q[0], axis=0, keepdims=True),
            jnp.where(sk == 2, total[0:1], 0),
        ),
    )
    ysv = ys[...]
    small = lane_scan(jnp.concatenate([ysv, hy[...], lines, total, q[0]], 0))[:, end]
    ends_of = jnp.broadcast_to(small[2 * ni : 2 * ni + SUB], (SUB, nl))
    whole, first_j, first_i = (ends_of[r : r + 1] for r in (0, 2, 1))
    pk[0:SUB] = stacked([
        along(small[:ni]), whole, along(ysv[:, 0:1]),
        jnp.broadcast_to(lines[0:1, 0:1], (1, nl)), in_order(small[:ni], 2),
        in_order(small[ni : 2 * ni], 3),
    ])
    pk[SUB:] = lines + stacked([
        0, 0, 0, jnp.where(within(0) | within(2), whole, 0),
        jnp.where(within(3), first_j, 0), jnp.where(within(1), first_i, 0),
    ])


    outgoing = [
        (inside(X + dx, Y + dy), functools.partial(plane_copy, n))
        for n, (dx, dy) in enumerate(plane_to)
    ] + [
        (inside(X + dx, Y + dy, Z - 1), functools.partial(level_copy, n))
        for n, (dx, dy) in enumerate(level_to)
    ]
    outgoing += [
        (inside(X + dx, Y), functools.partial(beside_copy, n)) for n, dx in enumerate(beside)
    ]
    outgoing += ups("gx", xs, xup, xss, xrs) + downs("gx", q.at[0], xdn, 0)
    outgoing += downs("gy", hy, ydn, 1) + ups("gy", ys, yup, yss, yrs)
    relays = [
        (base, (Z > 0) & (Z + base < nz) & (first_y == (base == 2)))
        for base in (1, 2) if nz > base + 1
    ]

    def burst(before=()):
        pl.semaphore_wait(barrier, awaited)
        for here, copy in [*before, *outgoing]:
            send(here, copy)
        for base, here in relays:
            @pl.when(here)
            def _(base=base):
                greet({"gz": Z - 1}, ready.at[base - 1])

    first = 2 * ni + SUB
    px[0:SUB] = j_scan(packed(small[first : first + nj]))
    px[SUB : 2 * SUB] = j_scan(packed(total[:, 0:1]))
    px[2 * SUB :] = stacked([
        in_order(small[first : first + nj], 0), in_order(small[first + nj :], 1)
    ])
    @pl.when(jnp.logical_not(first_y))
    def _():
        burst()

    deep = min(DEEP, ni)

    def scan_block(g, _):
        part = q[pl.ds(g * deep, deep)].reshape(deep * nj, nk)
        scan[pl.ds(g * deep, deep)] = lane_scan(part).reshape(deep, nj, nk)
        return 0

    lax.fori_loop(0, ni // deep, scan_block, 0)

    def columns(source, column):
        w = jnp.zeros((SUB, nl), I32)
        for i in range(ni):
            for b in range(nb):
                part = source[i, b * SUB : (b + 1) * SUB, column]
                w = jnp.where(lanes == i * nb + b, part, w)
        return i_scan(j_scan(w))

    ds[...] = columns(q, slice(0, 1))
    [(below, down_ds)] = downs("gz", ds, zdn, 2)

    @pl.when(first_y)
    def _():
        burst([(below, down_ds)])

    send(below & jnp.logical_not(first_y), down_ds)
    a0 = columns(scan, end)

    def hear(d, also):
        @pl.when((Z + d < nz) & also & (True if d > 2 else jnp.logical_not(first_y)))
        def _():
            pl.semaphore_wait(ready.at[d - 2], 1)

            if d < nz - 1:
                @pl.when(Z > 0)
                def _():
                    greet({"gz": Z - 1}, ready.at[d - 1])

    for d in range(2, nz):
        hear(d, Z > 0)

    for n, dx in enumerate(beside):
        @pl.when(inside(X - dx, Y))
        def _(n=n):
            beside_copy(n).wait_recv()

    xa = pxin[1, 0:SUB]
    for n in range(2, nx):
        xa = xa + pxin[n, 0:SUB]
    a0 = a0 + xa
    borders = pxin[0, 2 * SUB + 1 : 2 * SUB + 2]
    for n in range(1, nx):
        borders = borders + pxin[n, 2 * SUB : 2 * SUB + 1]
    z_refs = (zs, zup, zss, zrs)
    higher = ups("gz", *z_refs)
    higher_rows = ups("gz", zr, zrin, rss, rrs)
    up_wait("gx", xs, xup, xss, xrs)
    down_wait("gx", q.at[0], xdn, 0)
    rxv = xup[0]
    for d in range(1, nx - 1):
        rxv = rxv + xup[d]
    lx = lane_scan(jnp.concatenate([rxv, xdn[...]], 0))
    ax[...] = row_scan(lx[:nj])
    hxc[...] = row_scan(lx[nj:])

    def sweep_all():
        jrow = iota((nj, nk), 0)
        klane = iota((nj, nk), 1)
        plane = ax[...]

        def field(i, before):
            inner = before + row_scan(scan[i])
            return inner, inner + plane + by[pl.ds(i, 1), :]

        def stencil(i, low, mid, high):
            down_j = jnp.where(jrow == 0, by[pl.ds(i, 1), :], turn(mid, 1, 0))
            edge_j = jnp.where(last_y, 0, mid)
            up_j = jnp.where(jrow == nj - 1, edge_j, turn(mid, nj - 1, 0))
            down_k = jnp.where(klane == 0, 0, turn(mid, 1, 1))
            edge_k = jnp.where(last_z, 0, mid)
            up_k = jnp.where(klane == nk - 1, edge_k, turn(mid, nk - 1, 1))
            v_ref[i] = 6 * mid + (low + high) + (down_j + up_j) + (down_k + up_k)

        def sweep(i, state):
            low, mid, before = state
            inner, high = field(i + 1, before)
            stencil(i, low, mid, high)
            return mid, high, inner

        inner, mid = field(0, jnp.zeros((nj, nk), I32))
        state = (plane + tails[0:1], mid, inner)
        many = (ni - 1) // UNROLL

        def sweeps(g, state):
            for u in range(UNROLL):
                state = sweep(g * UNROLL + u, state)
            return state

        state = lax.fori_loop(0, many, sweeps, state)
        for i in range(many * UNROLL, ni - 1):
            state = sweep(i, state)
        low, mid, _ = state
        stencil(ni - 1, low, mid, jnp.where(last_x, 0, mid + hxc[...] + tails[1:2]))

    @pl.when(first_y)
    def _():
        tails[...] = jnp.zeros_like(tails)
        by[...] = jnp.zeros_like(by)
        zs[...] = a0
        for here, copy in higher[-2:]:
            send(here, copy)
        sweep_all()
        for d in range(3, nz):
            hear(d, Z == 0)
        for here, copy in higher[:-2]:
            send(here, copy)

    for n, (dx, dy) in enumerate(plane_to):
        @pl.when(inside(X - dx, Y - dy))
        def _(n=n):
            plane_copy(n).wait_recv()

    def gather(wanted, slots):
        found = [slots(n) for n, m in enumerate(plane_to) if wanted(*m)]
        return functools.reduce(jnp.add, found) if found else jnp.zeros((SUB, nk), I32)

    kinds = (
        (lambda dx, dy: dx == 0 and dy > 0, 4), (lambda dx, dy: dx > 0 and dy > 0, SUB + 3),
        (lambda dx, dy: dx == 0 and dy < 0, 5), (lambda dx, dy: dx > 0 and dy < 0, SUB + 4),
        (lambda dx, dy: dx < 0, SUB + 5),
    )
    for wanted, r in kinds:
        at = r // SUB * SUB
        borders = borders + gather(wanted, lambda n: pkin[n, at : at + SUB])[r - at : r - at + 1]
    zr[...] = borders

    @pl.when(jnp.logical_not(first_y))
    def _():
        low, corner = (gather(kinds[k][0], lambda n: pkin[n, 0:SUB]) for k in (0, 1))
        zs[...] = a0 + (low[0:1] + corner[1:2])
        for d in range(2, nz):
            hear(d, Z == 0)
        for here, copy in higher:
            send(here, copy)

    for here, copy in higher_rows:
        send(here, copy)

    up_wait("gy", ys, yup, yss, yrs)
    down_wait("gy", hy, ydn, 1)
    ryv = yup[0]
    for d in range(1, ny - 1):
        ryv = ryv + yup[d]
    rytv = stacked([
        gather(kinds[k][0], lambda n: pkin[n, SUB:])[r : r + 1] for r, k in enumerate((1, 4, 3))
    ])
    ly = lane_scan(jnp.concatenate([ryv, ydn[...], rytv], 0))
    lyl, lyh, lyt = ly[:ni], ly[ni : 2 * ni], ly[2 * ni :]
    rows_i = iota((ni, nk), 0)
    hyc[...] = row_scan(lyh + jnp.where(rows_i == 0, lyt[2:3], 0))

    @pl.when(jnp.logical_not(first_y))
    def _():
        tails[...] = lyt
        by[...] = row_scan(lyl + jnp.where(rows_i == 0, lyt[0:1], 0))
        sweep_all()

    for i in range(ni):
        beyond_j = jnp.where(sk == SUB - 1, hyc[pl.ds(i, 1), :], 0)
        v_ref[i, nj - SUB : nj, :] += jnp.where(last_y, 0, beyond_j)

    finish_sends([*outgoing, (below, down_ds)])
    for n, (dx, dy) in enumerate(level_to):
        @pl.when(inside(X - dx, Y - dy, Z + 1))
        def _(n=n):
            level_copy(n).wait_recv()

    down_wait("gz", ds, zdn, 2)
    up_wait("gz", *z_refs)
    up_wait("gz", zr, zrin, rss, rrs)
    beyond = zdn[...]
    for n, (dx, dy) in enumerate(level_to):
        r = 2 if dx == 0 else 3
        beyond = beyond + (dgin[n, r : r + 1, :] if dy else dgin[n])
    D, borders = zup[0], zrin[0]
    for d in range(1, nz - 1):
        D, borders = D + zup[d], borders + zrin[d]
    borders = jnp.broadcast_to(borders, D.shape)

    def pick(index):
        return jnp.take_along_axis(borders, index, 1, mode="promise_in_bounds")

    front, back = pick(block * SUB + subs), pick(nj + block * SUB + subs)
    prior, after = pltpu.roll(D, 1, 0), pltpu.roll(D, SUB - 1, 0)

    def finals(by):
        at = lax.rem(lanes + (nl - by), nl)
        moved_to = lambda w, d: turn(w, d + by, 1)
        here = moved_to(D, 0)
        y_low, y_high = (pick(starts[k] + at // nb) for k in (2, 3))
        down_i = jnp.where(at < nb, front, moved_to(D, nb))
        edge_i = jnp.where(last_x, 0, here + back)
        up_i = jnp.where(at >= nl - nb, edge_i, moved_to(D, nl - nb))
        edge_j = jnp.where(block == 0, y_low, moved_to(prior, 1))
        down_j = jnp.where(subs == 0, edge_j, moved_to(prior, 0))
        edge_j = jnp.where(last_y, 0, here + y_high)
        edge_j = jnp.where(block == nb - 1, edge_j, moved_to(after, nl - 1))
        up_j = jnp.where(subs == SUB - 1, edge_j, moved_to(after, 0))
        E = 8 * here + (down_i + up_i) + (down_j + up_j)
        return E, E + jnp.where(last_z, -here, moved_to(beyond, 0))

    E, EH = finals(0)
    E_half, EH_half = finals(half)
    eh_ref[0:SUB] = jnp.where(lanes < half, E, EH_half)
    eh_ref[SUB : 2 * SUB] = jnp.where(lanes < half, E_half, EH)

    finish_sends([*higher, *higher_rows])


def messages(nx, ny):
    plane = [(dx, -1) for dx in range(nx)] + [
        (dx, dy) for dy in range(ny - 1, 0, -1) for dx in range(-1, nx)
    ]
    level = [(dx, dy) for dy in range(ny - 1, -1, -1) for dx in range(nx) if dx or dy]
    return plane, level


def finish(step_ref, v_ref, eh_ref, out_hbm, out, sems):
    ni, nj, nk = out.shape
    nb = nj // SUB
    scale = step_ref[0] * (1.0 / 12.0)
    half = ni * nb // 2
    base = jnp.where(iota((SUB, nk), 1) == nk - 1, half, 0)
    halves = eh_ref[0:SUB], eh_ref[SUB : 2 * SUB]
    steps = sems.shape[0] // 2
    depth = ni // 2 // steps
    turned = [[turn(w, half * 2 - c, 1) for c in range(TURNS)] for w in halves]
    copies = []
    for p in range(steps):
        for i in range(p * depth, (p + 1) * depth):
            for b in range(nb):
                v = i * nb + b
                c = v % TURNS
                rows = slice(b * SUB, (b + 1) * SUB)
                for at, source in ((i, turned[0][c]), (i + ni // 2, turned[1][c])):
                    carry = jnp.take_along_axis(
                        source, base + (v - c), 1, mode="promise_in_bounds"
                    )
                    out[at, rows, :] = (v_ref[at, rows, :] + carry).astype(F32) * scale
        for h in range(2):
            part = pl.ds(h * (ni // 2) + p * depth, depth)
            copy = pltpu.make_async_copy(out.at[part], out_hbm.at[part], sems.at[2 * p + h])
            copy.start()
            copies.append(copy)
    for copy in copies:
        copy.wait()


def solution(mesh):
    sizes = tuple(mesh.shape[a] for a in ("gx", "gy", "gz"))
    nx, ny, nz = sizes

    def on_device(quant_codes, error_step):
        ni, nj, nk = quant_codes.shape
        nl = ni * nj // SUB
        vm = lambda *shape: pltpu.VMEM(shape, I32)
        dma = lambda n: pltpu.SemaphoreType.DMA((n,))
        plane_to, level_to = messages(nx, ny)
        np_, ng = len(plane_to), len(level_to)
        scratch = [
            vm(ni, nj, nk), vm(ni, nj, nk),
            vm(nj, nk), vm(nx - 1, nj, nk), vm(nj, nk),
            vm(ni, nk), vm(ny - 1, ni, nk), vm(ni, nk), vm(ni, nk),
            vm(2 * SUB, nl), vm(np_, 2 * SUB, nl), vm(3 * SUB, nl), vm(nx, 3 * SUB, nl),
            vm(ng, SUB, nl),
            vm(SUB, nl), vm(nz - 1, SUB, nl), vm(1, nl), vm(nz - 1, 1, nl),
            vm(SUB, nl), vm(SUB, nl),
            vm(nj, nk), vm(nj, nk), vm(ni, nk), vm(ni, nk), vm(SUB, nk),
        ]
        semaphores = [
            pltpu.SemaphoreType.DMA,
            dma(nx - 1), dma(nx - 1), dma(ny - 1), dma(ny - 1),
            dma(np_), dma(np_), dma(nx), dma(nx), dma(ng), dma(ng), *[dma(nz - 1)] * 4,
            dma(3), dma(3),
            pltpu.SemaphoreType.REGULAR((max(nz - 2, 1),)),
        ]

        def scoped(*refs):
            def body(*sems):
                exchange(sizes, *refs, *sems)

            pl.run_scoped(body, *semaphores)

        any_space = pl.BlockSpec(memory_space=pl.ANY)
        hbm = pl.BlockSpec(memory_space=pltpu.HBM)
        vmem = pl.BlockSpec(memory_space=pltpu.VMEM)
        v, eh = pl.pallas_call(
            scoped,
            out_shape=(
                jax.ShapeDtypeStruct((ni, nj, nk), I32),
                jax.ShapeDtypeStruct((2 * SUB, nl), I32),
            ),
            in_specs=[hbm],
            out_specs=(vmem, vmem),
            scratch_shapes=scratch,
            compiler_params=pltpu.CompilerParams(
                collective_id=0, has_side_effects=True, vmem_limit_bytes=GRANT
            ),
            name="exchange",
        )(pltpu.with_memory_space_constraint(quant_codes, pltpu.HBM))
        return pl.pallas_call(
            finish,
            out_shape=jax.ShapeDtypeStruct((ni, nj, nk), F32),
            in_specs=[pl.BlockSpec(memory_space=pltpu.SMEM), vmem, vmem],
            out_specs=any_space,
            scratch_shapes=[pltpu.VMEM((ni, nj, nk), F32), dma(8)],
            compiler_params=pltpu.CompilerParams(vmem_limit_bytes=16 * 2**20),
            name="finish",
        )(error_step, v, eh)

    return jax.shard_map(
        on_device, mesh=mesh, in_specs=(P("gx", "gy", "gz"), P()),
        out_specs=P("gx", "gy", "gz"), check_vma=False,
    )
```

```python
import functools

import jax
import jax.numpy as jnp
from jax import lax
from jax.experimental import pallas as pl
from jax.experimental.pallas import tpu as pltpu
from jax.sharding import PartitionSpec as P

MESH = pl.DeviceIdType.MESH
I32 = jnp.int32
F32 = jnp.float32
SUB = 8
GRANT = 16 * 2**20
UNROLL = 4
DEEP = 16
TURNS = 8


def iota(shape, dim):
    return lax.broadcasted_iota(I32, shape, dim)


def turn(x, by, dim):
    n = x.shape[dim]
    by = by % n
    if by == 0:
        return x
    if dim == 1 and n % 128 != 0:
        return jnp.concatenate([x[:, n - by :], x[:, : n - by]], 1)
    return pltpu.roll(x, by, dim)


def lane_scan(x):
    n = x.shape[1]
    tri = (iota((n, n), 0) <= iota((n, n), 1)).astype(F32)
    one, big = tri.astype(jnp.bfloat16), (tri * 256.0).astype(jnp.bfloat16)

    def times(part, m):
        return jnp.dot(part.astype(F32).astype(jnp.bfloat16), m, preferred_element_type=F32)

    low = times(x & 255, one) + times((x >> 8) & 255, big)
    high = times((x >> 16) & 255, one) + times(x >> 24, big)
    return low.astype(I32) + (high.astype(I32) << 16)


def row_scan(x):
    rows, n = x.shape
    s = iota((SUB, n), 0)
    out, carry = [], None
    for b in range(rows // SUB):
        v = x[b * SUB : (b + 1) * SUB]
        for d in (1, 2, 4):
            v = v + jnp.where(s >= d, pltpu.roll(v, d, 0), 0)
        if carry is not None:
            v = v + carry
        carry = jnp.broadcast_to(v[SUB - 1 : SUB], (SUB, n))
        out.append(v)
    return jnp.concatenate(out, 0) if len(out) > 1 else out[0]


def exchange(
    mesh_sizes, q_hbm, v_ref, eh_ref,
    q, scan, xs, xup, xdn, ys, yup, hy, ydn, pk, pkin, px, pxin, dgin,
    zs, zup, zr, zrin, ds, zdn, ax, hxc, by, hyc, tails,
    load_sem, xss, xrs, yss, yrs, pss, prs, ass, ars, gss, grs, zss, zrs, rss, rrs, dss, drs, ready,
):
    nx, ny, nz = mesh_sizes
    ni, nj, nk = q.shape
    nb = nj // SUB
    nl = ni * nb
    X, Y, Z = (lax.axis_index(a) for a in ("gx", "gy", "gz"))
    place = {"gx": X, "gy": Y, "gz": Z}
    size = {"gx": nx, "gy": ny, "gz": nz}
    last_x, last_y, last_z = X == nx - 1, Y == ny - 1, Z == nz - 1
    plane_to, level_to = messages(nx, ny)
    beside = [-1, *range(1, nx)]

    load = pltpu.make_async_copy(q_hbm, q, load_sem)
    load.start()
    barrier = pltpu.get_barrier_semaphore()

    def greet(to, sem):
        pl.semaphore_signal(sem, inc=1, device_id=to, device_id_type=MESH)

    def inside(x, y, z=0):
        ok = (x >= 0) & (x < nx) & (y >= 0) & (y < ny)
        return ok if isinstance(z, int) else ok & (z >= 0) & (z < nz)

    def greet_plane(dx, dy):
        greet({"gx": lax.rem(X + dx, nx), "gy": lax.rem(Y + dy, ny)}, barrier)

    for dy in range(1, ny):
        greet_plane(0, dy)
    first_y = Y == 0
    for d in (-2, -1, 1):
        @pl.when((Z + d >= 0) & (Z + d < nz) & (first_y if d == -2 else True))
        def _(d=d):
            greet({"gz": Z + d}, barrier)

    for dx in range(1, nx):
        for dy in range(ny):
            greet_plane(dx, dy)

    for dx, dy in level_to:
        @pl.when(inside(X - dx, Y - dy, Z + 1))
        def _(dx=dx, dy=dy):
            greet({"gx": X - dx, "gy": Y - dy, "gz": Z + 1}, barrier)

    near = sum(((Z + d >= 0) & (Z + d < nz)).astype(I32) for d in (-1, 1))
    near = near + (first_y & (Z + 2 < nz)).astype(I32)
    above = jnp.where(Z > 0, (nx - X) * (ny - Y) - 1, 0)
    awaited = nx * ny - 1 + near + above

    def clear(here, slot):
        @pl.when(here)
        def _():
            slot[...] = jnp.zeros(slot.shape, I32)

    for n, (dx, dy) in enumerate(plane_to):
        clear(jnp.logical_not(inside(X - dx, Y - dy)), pkin.at[n])
    for n, dx in enumerate(beside):
        clear(jnp.logical_not(inside(X - dx, Y)), pxin.at[n])
    for n, (dx, dy) in enumerate(level_to):
        clear(jnp.logical_not(inside(X - dx, Y - dy, Z + 1)), dgin.at[n])
    for axis, slots, beyond in (("gx", xup, xdn), ("gy", yup, ydn), ("gz", zup, zdn), ("gz", zrin, None)):
        for d in range(1, size[axis]):
            clear(place[axis] < d, slots.at[d - 1])
        if beyond is not None:
            clear(place[axis] == size[axis] - 1, beyond)

    def send(here, copy):
        @pl.when(here)
        def _():
            copy().start()

    def finish_sends(started):
        for here, copy in started:
            @pl.when(here)
            def _(copy=copy):
                copy().wait_send()

    def up_copy(axis, src, slots, ssem, rsem, d):
        return pltpu.make_async_remote_copy(
            src_ref=src, dst_ref=slots.at[d - 1], send_sem=ssem.at[d - 1],
            recv_sem=rsem.at[d - 1], device_id={axis: place[axis] + d},
            device_id_type=MESH,
        )

    def ups(axis, *refs):
        return [
            (place[axis] + d < size[axis], functools.partial(up_copy, axis, *refs, d))
            for d in range(size[axis] - 1, 0, -1)
        ]

    def up_wait(axis, *refs):
        for d in range(1, size[axis]):
            @pl.when(place[axis] >= d)
            def _(d=d):
                up_copy(axis, *refs, d).wait_recv()

    def down_copy(axis, src, dst, n):
        return pltpu.make_async_remote_copy(
            src_ref=src, dst_ref=dst, send_sem=dss.at[n], recv_sem=drs.at[n],
            device_id={axis: place[axis] - 1}, device_id_type=MESH,
        )

    def downs(axis, src, dst, n):
        return [(place[axis] > 0, functools.partial(down_copy, axis, src, dst, n))]

    def down_wait(axis, src, dst, n):
        @pl.when(place[axis] < size[axis] - 1)
        def _():
            down_copy(axis, src, dst, n).wait_recv()

    def plane_copy(n):
        return pltpu.make_async_remote_copy(
            src_ref=pk if plane_to[n][0] else pk.at[0:SUB],
            dst_ref=pkin.at[n] if plane_to[n][0] else pkin.at[n, 0:SUB],
            send_sem=pss.at[n], recv_sem=prs.at[n],
            device_id={"gx": X + plane_to[n][0], "gy": Y + plane_to[n][1]},
            device_id_type=MESH,
        )

    def beside_copy(n):
        return pltpu.make_async_remote_copy(
            src_ref=px, dst_ref=pxin.at[n], send_sem=ass.at[n], recv_sem=ars.at[n],
            device_id={"gx": X + beside[n]}, device_id_type=MESH,
        )

    def level_copy(n):
        return pltpu.make_async_remote_copy(
            src_ref=pk.at[0:SUB] if level_to[n][1] else px.at[SUB : 2 * SUB],
            dst_ref=dgin.at[n], send_sem=gss.at[n],
            recv_sem=grs.at[n], device_id_type=MESH,
            device_id={"gx": X + level_to[n][0], "gy": Y + level_to[n][1], "gz": Z - 1},
        )

    lanes = iota((SUB, nl), 1)
    subs = iota((SUB, nl), 0)
    sk = iota((SUB, nk), 0)
    block = lax.rem(lanes, nb)
    half = nl // 2
    starts = (0, nj, 2 * nj, 2 * nj + ni, 2 * (nj + ni))
    lane = iota((1, nl), 1)

    def within(k):
        return (lane >= starts[k]) & (lane < starts[k + 1])

    def in_order(column, k):
        n = column.shape[0]
        at = iota((n, nl), 1) - starts[k]
        reached = (at >= iota((n, nl), 0)) & (at < n)
        return jnp.sum(jnp.where(reached, column, 0), axis=0, keepdims=True)
    end = slice(nk - 1, nk)
    upto = (iota((ni, nl), 1) // nb) >= iota((ni, nl), 0)

    def along(column):
        return jnp.sum(jnp.where(upto, column, 0), axis=0, keepdims=True)

    def j_scan(w):
        for d in (1, 2, 4):
            w = w + jnp.where(subs >= d, pltpu.roll(w, d, 0), 0)
        whole = jnp.broadcast_to(w[SUB - 1 : SUB], w.shape)
        for d in range(1, nb):
            w = w + jnp.where(block >= d, turn(whole, d, 1), 0)
        return w

    def stacked(values):
        w = jnp.zeros((SUB, nl), I32)
        for r, value in enumerate(values):
            w = jnp.where(subs == r, value, w)
        return w

    def packed(column):
        w = jnp.zeros((SUB, nl), I32)
        for b in range(nb):
            w = jnp.where(block == b, column[b * SUB : (b + 1) * SUB], w)
        return w

    def i_scan(w):
        d = nb
        while d < nl:
            w = w + jnp.where(lanes >= d, turn(w, d, 1), 0)
            d *= 2
        return w

    load.wait()
    total = q[0]
    for i in range(1, ni):
        total = total + q[i]
    xs[...] = total
    for i in range(ni):
        ys[pl.ds(i, 1), :] = jnp.sum(q[i], axis=0, keepdims=True)
        hy[pl.ds(i, 1), :] = q[i, 0:1, :]
    lines = jnp.where(
        sk == 0, jnp.sum(total, axis=0, keepdims=True),
        jnp.where(
            sk == 1, jnp.sum(q[0], axis=0, keepdims=True),
            jnp.where(sk == 2, total[0:1], 0),
        ),
    )
    ysv = ys[...]
    small = lane_scan(jnp.concatenate([ysv, hy[...], lines, total, q[0]], 0))[:, end]
    ends_of = jnp.broadcast_to(small[2 * ni : 2 * ni + SUB], (SUB, nl))
    whole, first_j, first_i = (ends_of[r : r + 1] for r in (0, 2, 1))
    pk[0:SUB] = stacked([
        along(small[:ni]), whole, along(ysv[:, 0:1]),
        jnp.broadcast_to(lines[0:1, 0:1], (1, nl)), in_order(small[:ni], 2),
        in_order(small[ni : 2 * ni], 3),
    ])
    pk[SUB:] = lines + stacked([
        0, 0, 0, jnp.where(within(0) | within(2), whole, 0),
        jnp.where(within(3), first_j, 0), jnp.where(within(1), first_i, 0),
    ])


    outgoing = [
        (inside(X + dx, Y + dy), functools.partial(plane_copy, n))
        for n, (dx, dy) in enumerate(plane_to)
    ] + [
        (inside(X + dx, Y + dy, Z - 1), functools.partial(level_copy, n))
        for n, (dx, dy) in enumerate(level_to)
    ]
    outgoing += [
        (inside(X + dx, Y), functools.partial(beside_copy, n)) for n, dx in enumerate(beside)
    ]
    outgoing += ups("gx", xs, xup, xss, xrs) + downs("gx", q.at[0], xdn, 0)
    outgoing += downs("gy", hy, ydn, 1) + ups("gy", ys, yup, yss, yrs)
    relays = [
        (base, (Z > 0) & (Z + base < nz) & (first_y == (base == 2)))
        for base in (1, 2) if nz > base + 1
    ]

    def burst(before=()):
        pl.semaphore_wait(barrier, awaited)
        for here, copy in [*before, *outgoing]:
            send(here, copy)
        for base, here in relays:
            @pl.when(here)
            def _(base=base):
                greet({"gz": Z - 1}, ready.at[base - 1])

    first = 2 * ni + SUB
    px[0:SUB] = j_scan(packed(small[first : first + nj]))
    px[SUB : 2 * SUB] = j_scan(packed(total[:, 0:1]))
    px[2 * SUB :] = stacked([
        in_order(small[first : first + nj], 0), in_order(small[first + nj :], 1)
    ])
    @pl.when(jnp.logical_not(first_y))
    def _():
        burst()

    deep = min(DEEP, ni)

    def scan_block(g, _):
        part = q[pl.ds(g * deep, deep)].reshape(deep * nj, nk)
        scan[pl.ds(g * deep, deep)] = lane_scan(part).reshape(deep, nj, nk)
        return 0

    lax.fori_loop(0, ni // deep, scan_block, 0)

    def columns(source, column):
        w = jnp.zeros((SUB, nl), I32)
        for i in range(ni):
            for b in range(nb):
                part = source[i, b * SUB : (b + 1) * SUB, column]
                w = jnp.where(lanes == i * nb + b, part, w)
        return i_scan(j_scan(w))

    ds[...] = columns(q, slice(0, 1))
    [(below, down_ds)] = downs("gz", ds, zdn, 2)

    @pl.when(first_y)
    def _():
        burst([(below, down_ds)])

    send(below & jnp.logical_not(first_y), down_ds)
    a0 = columns(scan, end)

    def hear(d, also):
        @pl.when((Z + d < nz) & also & (True if d > 2 else jnp.logical_not(first_y)))
        def _():
            pl.semaphore_wait(ready.at[d - 2], 1)

            if d < nz - 1:
                @pl.when(Z > 0)
                def _():
                    greet({"gz": Z - 1}, ready.at[d - 1])

    for d in range(2, nz):
        hear(d, Z > 0)

    for n, dx in enumerate(beside):
        @pl.when(inside(X - dx, Y))
        def _(n=n):
            beside_copy(n).wait_recv()

    xa = pxin[1, 0:SUB]
    for n in range(2, nx):
        xa = xa + pxin[n, 0:SUB]
    a0 = a0 + xa
    borders = pxin[0, 2 * SUB + 1 : 2 * SUB + 2]
    for n in range(1, nx):
        borders = borders + pxin[n, 2 * SUB : 2 * SUB + 1]
    z_refs = (zs, zup, zss, zrs)
    higher = ups("gz", *z_refs)
    higher_rows = ups("gz", zr, zrin, rss, rrs)
    up_wait("gx", xs, xup, xss, xrs)
    down_wait("gx", q.at[0], xdn, 0)
    rxv = xup[0]
    for d in range(1, nx - 1):
        rxv = rxv + xup[d]
    lx = lane_scan(jnp.concatenate([rxv, xdn[...]], 0))
    ax[...] = row_scan(lx[:nj])
    hxc[...] = row_scan(lx[nj:])

    def sweep_all():
        jrow = iota((nj, nk), 0)
        klane = iota((nj, nk), 1)
        plane = ax[...]

        def field(i, before):
            inner = before + row_scan(scan[i])
            return inner, inner + plane + by[pl.ds(i, 1), :]

        def stencil(i, low, mid, high):
            down_j = jnp.where(jrow == 0, by[pl.ds(i, 1), :], turn(mid, 1, 0))
            edge_j = jnp.where(last_y, 0, mid)
            up_j = jnp.where(jrow == nj - 1, edge_j, turn(mid, nj - 1, 0))
            down_k = jnp.where(klane == 0, 0, turn(mid, 1, 1))
            edge_k = jnp.where(last_z, 0, mid)
            up_k = jnp.where(klane == nk - 1, edge_k, turn(mid, nk - 1, 1))
            v_ref[i] = 6 * mid + (low + high) + (down_j + up_j) + (down_k + up_k)

        def sweep(i, state):
            low, mid, before = state
            inner, high = field(i + 1, before)
            stencil(i, low, mid, high)
            return mid, high, inner

        inner, mid = field(0, jnp.zeros((nj, nk), I32))
        state = (plane + tails[0:1], mid, inner)
        many = (ni - 1) // UNROLL

        def sweeps(g, state):
            for u in range(UNROLL):
                state = sweep(g * UNROLL + u, state)
            return state

        state = lax.fori_loop(0, many, sweeps, state)
        for i in range(many * UNROLL, ni - 1):
            state = sweep(i, state)
        low, mid, _ = state
        stencil(ni - 1, low, mid, jnp.where(last_x, 0, mid + hxc[...] + tails[1:2]))

    @pl.when(first_y)
    def _():
        tails[...] = jnp.zeros_like(tails)
        by[...] = jnp.zeros_like(by)
        zs[...] = a0
        for here, copy in higher[-2:]:
            send(here, copy)
        sweep_all()
        for d in range(3, nz):
            hear(d, Z == 0)
        for here, copy in higher[:-2]:
            send(here, copy)

    for n, (dx, dy) in enumerate(plane_to):
        @pl.when(inside(X - dx, Y - dy))
        def _(n=n):
            plane_copy(n).wait_recv()

    def gather(wanted, slots):
        found = [slots(n) for n, m in enumerate(plane_to) if wanted(*m)]
        return functools.reduce(jnp.add, found) if found else jnp.zeros((SUB, nk), I32)

    kinds = (
        (lambda dx, dy: dx == 0 and dy > 0, 4), (lambda dx, dy: dx > 0 and dy > 0, SUB + 3),
        (lambda dx, dy: dx == 0 and dy < 0, 5), (lambda dx, dy: dx > 0 and dy < 0, SUB + 4),
        (lambda dx, dy: dx < 0, SUB + 5),
    )
    for wanted, r in kinds:
        at = r // SUB * SUB
        borders = borders + gather(wanted, lambda n: pkin[n, at : at + SUB])[r - at : r - at + 1]
    zr[...] = borders

    @pl.when(jnp.logical_not(first_y))
    def _():
        low, corner = (gather(kinds[k][0], lambda n: pkin[n, 0:SUB]) for k in (0, 1))
        zs[...] = a0 + (low[0:1] + corner[1:2])
        for d in range(2, nz):
            hear(d, Z == 0)
        for here, copy in higher:
            send(here, copy)

    for here, copy in higher_rows:
        send(here, copy)

    up_wait("gy", ys, yup, yss, yrs)
    down_wait("gy", hy, ydn, 1)
    ryv = yup[0]
    for d in range(1, ny - 1):
        ryv = ryv + yup[d]
    rytv = stacked([
        gather(kinds[k][0], lambda n: pkin[n, SUB:])[r : r + 1] for r, k in enumerate((1, 4, 3))
    ])
    ly = lane_scan(jnp.concatenate([ryv, ydn[...], rytv], 0))
    lyl, lyh, lyt = ly[:ni], ly[ni : 2 * ni], ly[2 * ni :]
    rows_i = iota((ni, nk), 0)
    hyc[...] = row_scan(lyh + jnp.where(rows_i == 0, lyt[2:3], 0))

    @pl.when(jnp.logical_not(first_y))
    def _():
        tails[...] = lyt
        by[...] = row_scan(lyl + jnp.where(rows_i == 0, lyt[0:1], 0))
        sweep_all()

    for i in range(ni):
        beyond_j = jnp.where(sk == SUB - 1, hyc[pl.ds(i, 1), :], 0)
        v_ref[i, nj - SUB : nj, :] += jnp.where(last_y, 0, beyond_j)

    finish_sends([*outgoing, (below, down_ds)])
    for n, (dx, dy) in enumerate(level_to):
        @pl.when(inside(X - dx, Y - dy, Z + 1))
        def _(n=n):
            level_copy(n).wait_recv()

    down_wait("gz", ds, zdn, 2)
    up_wait("gz", *z_refs)
    up_wait("gz", zr, zrin, rss, rrs)
    beyond = zdn[...]
    for n, (dx, dy) in enumerate(level_to):
        r = 2 if dx == 0 else 3
        beyond = beyond + (dgin[n, r : r + 1, :] if dy else dgin[n])
    D, borders = zup[0], zrin[0]
    for d in range(1, nz - 1):
        D, borders = D + zup[d], borders + zrin[d]
    borders = jnp.broadcast_to(borders, D.shape)

    def pick(index):
        return jnp.take_along_axis(borders, index, 1, mode="promise_in_bounds")

    front, back = pick(block * SUB + subs), pick(nj + block * SUB + subs)
    prior, after = pltpu.roll(D, 1, 0), pltpu.roll(D, SUB - 1, 0)

    def finals(by):
        at = lax.rem(lanes + (nl - by), nl)
        moved_to = lambda w, d: turn(w, d + by, 1)
        here = moved_to(D, 0)
        y_low, y_high = (pick(starts[k] + at // nb) for k in (2, 3))
        down_i = jnp.where(at < nb, front, moved_to(D, nb))
        edge_i = jnp.where(last_x, 0, here + back)
        up_i = jnp.where(at >= nl - nb, edge_i, moved_to(D, nl - nb))
        edge_j = jnp.where(block == 0, y_low, moved_to(prior, 1))
        down_j = jnp.where(subs == 0, edge_j, moved_to(prior, 0))
        edge_j = jnp.where(last_y, 0, here + y_high)
        edge_j = jnp.where(block == nb - 1, edge_j, moved_to(after, nl - 1))
        up_j = jnp.where(subs == SUB - 1, edge_j, moved_to(after, 0))
        E = 8 * here + (down_i + up_i) + (down_j + up_j)
        return E, E + jnp.where(last_z, -here, moved_to(beyond, 0))

    E, EH = finals(0)
    E_half, EH_half = finals(half)
    eh_ref[0:SUB] = jnp.where(lanes < half, E, EH_half)
    eh_ref[SUB : 2 * SUB] = jnp.where(lanes < half, E_half, EH)

    finish_sends([*higher, *higher_rows])


def messages(nx, ny):
    plane = [(dx, -1) for dx in range(nx)] + [
        (dx, dy) for dy in range(ny - 1, 0, -1) for dx in range(-1, nx)
    ]
    level = [(dx, dy) for dy in range(ny - 1, -1, -1) for dx in range(nx) if dx or dy]
    return plane, level


def finish(step_ref, v_ref, eh_ref, out_hbm, out, sems):
    ni, nj, nk = out.shape
    nb = nj // SUB
    scale = step_ref[0] * (1.0 / 12.0)
    half = ni * nb // 2
    base = jnp.where(iota((SUB, nk), 1) == nk - 1, half, 0)
    halves = eh_ref[0:SUB], eh_ref[SUB : 2 * SUB]
    steps = sems.shape[0] // 2
    depth = ni // 2 // steps
    turned = [[turn(w, half * 2 - c, 1) for c in range(TURNS)] for w in halves]
    copies = []
    for p in range(steps):
        for i in range(p * depth, (p + 1) * depth):
            for b in range(nb):
                v = i * nb + b
                c = v % TURNS
                rows = slice(b * SUB, (b + 1) * SUB)
                for at, source in ((i, turned[0][c]), (i + ni // 2, turned[1][c])):
                    carry = jnp.take_along_axis(
                        source, base + (v - c), 1, mode="promise_in_bounds"
                    )
                    out[at, rows, :] = (v_ref[at, rows, :] + carry).astype(F32) * scale
        for h in range(2):
            part = pl.ds(h * (ni // 2) + p * depth, depth)
            copy = pltpu.make_async_copy(out.at[part], out_hbm.at[part], sems.at[2 * p + h])
            copy.start()
            copies.append(copy)
    for copy in copies:
        copy.wait()


def solution(mesh):
    sizes = tuple(mesh.shape[a] for a in ("gx", "gy", "gz"))
    nx, ny, nz = sizes

    def on_device(quant_codes, error_step):
        ni, nj, nk = quant_codes.shape
        nl = ni * nj // SUB
        vm = lambda *shape: pltpu.VMEM(shape, I32)
        dma = lambda n: pltpu.SemaphoreType.DMA((n,))
        plane_to, level_to = messages(nx, ny)
        np_, ng = len(plane_to), len(level_to)
        scratch = [
            vm(ni, nj, nk), vm(ni, nj, nk),
            vm(nj, nk), vm(nx - 1, nj, nk), vm(nj, nk),
            vm(ni, nk), vm(ny - 1, ni, nk), vm(ni, nk), vm(ni, nk),
            vm(2 * SUB, nl), vm(np_, 2 * SUB, nl), vm(3 * SUB, nl), vm(nx, 3 * SUB, nl),
            vm(ng, SUB, nl),
            vm(SUB, nl), vm(nz - 1, SUB, nl), vm(1, nl), vm(nz - 1, 1, nl),
            vm(SUB, nl), vm(SUB, nl),
            vm(nj, nk), vm(nj, nk), vm(ni, nk), vm(ni, nk), vm(SUB, nk),
        ]
        semaphores = [
            pltpu.SemaphoreType.DMA,
            dma(nx - 1), dma(nx - 1), dma(ny - 1), dma(ny - 1),
            dma(np_), dma(np_), dma(nx), dma(nx), dma(ng), dma(ng), *[dma(nz - 1)] * 4,
            dma(3), dma(3),
            pltpu.SemaphoreType.REGULAR((max(nz - 2, 1),)),
        ]

        def scoped(*refs):
            def body(*sems):
                exchange(sizes, *refs, *sems)

            pl.run_scoped(body, *semaphores)

        any_space = pl.BlockSpec(memory_space=pl.ANY)
        hbm = pl.BlockSpec(memory_space=pltpu.HBM)
        vmem = pl.BlockSpec(memory_space=pltpu.VMEM)
        v, eh = pl.pallas_call(
            scoped,
            out_shape=(
                jax.ShapeDtypeStruct((ni, nj, nk), I32),
                jax.ShapeDtypeStruct((2 * SUB, nl), I32),
            ),
            in_specs=[hbm],
            out_specs=(vmem, vmem),
            scratch_shapes=scratch,
            compiler_params=pltpu.CompilerParams(
                collective_id=0, has_side_effects=True, vmem_limit_bytes=GRANT
            ),
            name="exchange",
        )(pltpu.with_memory_space_constraint(quant_codes, pltpu.HBM))
        def finish_scoped(*refs):
            pl.run_scoped(functools.partial(finish, *refs), dma(8))

        return pl.pallas_call(
            finish_scoped,
            out_shape=jax.ShapeDtypeStruct((ni, nj, nk), F32),
            in_specs=[pl.BlockSpec(memory_space=pltpu.SMEM), vmem, vmem],
            out_specs=any_space,
            scratch_shapes=[pltpu.VMEM((ni, nj, nk), F32)],
            compiler_params=pltpu.CompilerParams(vmem_limit_bytes=16 * 2**20),
            name="finish",
        )(error_step, v, eh)

    return jax.shard_map(
        on_device, mesh=mesh, in_specs=(P("gx", "gy", "gz"), P()),
        out_specs=P("gx", "gy", "gz"), check_vma=False,
    )
```

```python
import functools

import jax
import jax.numpy as jnp
from jax import lax
from jax.experimental import pallas as pl
from jax.experimental.pallas import tpu as pltpu
from jax.sharding import PartitionSpec as P

MESH = pl.DeviceIdType.MESH
I32 = jnp.int32
F32 = jnp.float32
SUB = 8
GRANT = 16 * 2**20
UNROLL = 4
DEEP = 16
TURNS = 8


def iota(shape, dim):
    return lax.broadcasted_iota(I32, shape, dim)


def turn(x, by, dim):
    n = x.shape[dim]
    by = by % n
    if by == 0:
        return x
    if dim == 1 and n % 128 != 0:
        return jnp.concatenate([x[:, n - by :], x[:, : n - by]], 1)
    return pltpu.roll(x, by, dim)


def lane_scan(x):
    n = x.shape[1]
    tri = (iota((n, n), 0) <= iota((n, n), 1)).astype(F32)
    one, big = tri.astype(jnp.bfloat16), (tri * 256.0).astype(jnp.bfloat16)

    def times(part, m):
        return jnp.dot(part.astype(F32).astype(jnp.bfloat16), m, preferred_element_type=F32)

    low = times(x & 255, one) + times((x >> 8) & 255, big)
    high = times((x >> 16) & 255, one) + times(x >> 24, big)
    return low.astype(I32) + (high.astype(I32) << 16)


def row_scan(x):
    rows, n = x.shape
    s = iota((SUB, n), 0)
    out, carry = [], None
    for b in range(rows // SUB):
        v = x[b * SUB : (b + 1) * SUB]
        for d in (1, 2, 4):
            v = v + jnp.where(s >= d, pltpu.roll(v, d, 0), 0)
        if carry is not None:
            v = v + carry
        carry = jnp.broadcast_to(v[SUB - 1 : SUB], (SUB, n))
        out.append(v)
    return jnp.concatenate(out, 0) if len(out) > 1 else out[0]


def exchange(
    mesh_sizes, q_hbm, v_ref, eh_ref,
    q, scan, xs, xup, xdn, ys, yup, hy, ydn, pk, pkin, px, pxin, dgin,
    zs, zup, zr, zrin, ds, zdn, ax, hxc, by, hyc, tails,
    load_sem, xss, xrs, yss, yrs, pss, prs, ass, ars, gss, grs, zss, zrs, rss, rrs, dss, drs, ready,
):
    nx, ny, nz = mesh_sizes
    ni, nj, nk = q.shape
    nb = nj // SUB
    nl = ni * nb
    X, Y, Z = (lax.axis_index(a) for a in ("gx", "gy", "gz"))
    place = {"gx": X, "gy": Y, "gz": Z}
    size = {"gx": nx, "gy": ny, "gz": nz}
    last_x, last_y, last_z = X == nx - 1, Y == ny - 1, Z == nz - 1
    plane_to, level_to = messages(nx, ny)
    beside = [-1, *range(1, nx)]

    load = pltpu.make_async_copy(q_hbm, q, load_sem)
    load.start()
    barrier = pltpu.get_barrier_semaphore()

    def greet(to, sem):
        pl.semaphore_signal(sem, inc=1, device_id=to, device_id_type=MESH)

    def inside(x, y, z=0):
        ok = (x >= 0) & (x < nx) & (y >= 0) & (y < ny)
        return ok if isinstance(z, int) else ok & (z >= 0) & (z < nz)

    def greet_plane(dx, dy):
        greet({"gx": lax.rem(X + dx, nx), "gy": lax.rem(Y + dy, ny)}, barrier)

    for dy in range(1, ny):
        greet_plane(0, dy)
    first_y = Y == 0
    for d in (-2, -1, 1):
        @pl.when((Z + d >= 0) & (Z + d < nz) & (first_y if d == -2 else True))
        def _(d=d):
            greet({"gz": Z + d}, barrier)

    for dx in range(1, nx):
        for dy in range(ny):
            greet_plane(dx, dy)

    for dx, dy in level_to:
        @pl.when(inside(X - dx, Y - dy, Z + 1))
        def _(dx=dx, dy=dy):
            greet({"gx": X - dx, "gy": Y - dy, "gz": Z + 1}, barrier)

    near = sum(((Z + d >= 0) & (Z + d < nz)).astype(I32) for d in (-1, 1))
    near = near + (first_y & (Z + 2 < nz)).astype(I32)
    above = jnp.where(Z > 0, (nx - X) * (ny - Y) - 1, 0)
    awaited = nx * ny - 1 + near + above

    def clear(here, slot):
        @pl.when(here)
        def _():
            slot[...] = jnp.zeros(slot.shape, I32)

    for n, (dx, dy) in enumerate(plane_to):
        clear(jnp.logical_not(inside(X - dx, Y - dy)), pkin.at[n])
    for n, dx in enumerate(beside):
        clear(jnp.logical_not(inside(X - dx, Y)), pxin.at[n])
    for n, (dx, dy) in enumerate(level_to):
        clear(jnp.logical_not(inside(X - dx, Y - dy, Z + 1)), dgin.at[n])
    for axis, slots, beyond in (("gx", xup, xdn), ("gy", yup, ydn), ("gz", zup, zdn), ("gz", zrin, None)):
        for d in range(1, size[axis]):
            clear(place[axis] < d, slots.at[d - 1])
        if beyond is not None:
            clear(place[axis] == size[axis] - 1, beyond)

    def send(here, copy):
        @pl.when(here)
        def _():
            copy().start()

    def finish_sends(started):
        for here, copy in started:
            @pl.when(here)
            def _(copy=copy):
                copy().wait_send()

    def up_copy(axis, src, slots, ssem, rsem, d):
        return pltpu.make_async_remote_copy(
            src_ref=src, dst_ref=slots.at[d - 1], send_sem=ssem.at[d - 1],
            recv_sem=rsem.at[d - 1], device_id={axis: place[axis] + d},
            device_id_type=MESH,
        )

    def ups(axis, *refs):
        return [
            (place[axis] + d < size[axis], functools.partial(up_copy, axis, *refs, d))
            for d in range(size[axis] - 1, 0, -1)
        ]

    def up_wait(axis, *refs):
        for d in range(1, size[axis]):
            @pl.when(place[axis] >= d)
            def _(d=d):
                up_copy(axis, *refs, d).wait_recv()

    def down_copy(axis, src, dst, n):
        return pltpu.make_async_remote_copy(
            src_ref=src, dst_ref=dst, send_sem=dss.at[n], recv_sem=drs.at[n],
            device_id={axis: place[axis] - 1}, device_id_type=MESH,
        )

    def downs(axis, src, dst, n):
        return [(place[axis] > 0, functools.partial(down_copy, axis, src, dst, n))]

    def down_wait(axis, src, dst, n):
        @pl.when(place[axis] < size[axis] - 1)
        def _():
            down_copy(axis, src, dst, n).wait_recv()

    def plane_copy(n):
        return pltpu.make_async_remote_copy(
            src_ref=pk if plane_to[n][0] else pk.at[0:SUB],
            dst_ref=pkin.at[n] if plane_to[n][0] else pkin.at[n, 0:SUB],
            send_sem=pss.at[n], recv_sem=prs.at[n],
            device_id={"gx": X + plane_to[n][0], "gy": Y + plane_to[n][1]},
            device_id_type=MESH,
        )

    def beside_copy(n):
        return pltpu.make_async_remote_copy(
            src_ref=px, dst_ref=pxin.at[n], send_sem=ass.at[n], recv_sem=ars.at[n],
            device_id={"gx": X + beside[n]}, device_id_type=MESH,
        )

    def level_copy(n):
        return pltpu.make_async_remote_copy(
            src_ref=pk.at[0:SUB] if level_to[n][1] else px.at[SUB : 2 * SUB],
            dst_ref=dgin.at[n], send_sem=gss.at[n],
            recv_sem=grs.at[n], device_id_type=MESH,
            device_id={"gx": X + level_to[n][0], "gy": Y + level_to[n][1], "gz": Z - 1},
        )

    lanes = iota((SUB, nl), 1)
    subs = iota((SUB, nl), 0)
    sk = iota((SUB, nk), 0)
    block = lax.rem(lanes, nb)
    half = nl // 2
    starts = (0, nj, 2 * nj, 2 * nj + ni, 2 * (nj + ni))
    lane = iota((1, nl), 1)

    def within(k):
        return (lane >= starts[k]) & (lane < starts[k + 1])

    def in_order(column, k):
        n = column.shape[0]
        at = iota((n, nl), 1) - starts[k]
        reached = (at >= iota((n, nl), 0)) & (at < n)
        return jnp.sum(jnp.where(reached, column, 0), axis=0, keepdims=True)
    end = slice(nk - 1, nk)
    upto = (iota((ni, nl), 1) // nb) >= iota((ni, nl), 0)

    def along(column):
        return jnp.sum(jnp.where(upto, column, 0), axis=0, keepdims=True)

    def j_scan(w):
        for d in (1, 2, 4):
            w = w + jnp.where(subs >= d, pltpu.roll(w, d, 0), 0)
        whole = jnp.broadcast_to(w[SUB - 1 : SUB], w.shape)
        for d in range(1, nb):
            w = w + jnp.where(block >= d, turn(whole, d, 1), 0)
        return w

    def stacked(values):
        w = jnp.zeros((SUB, nl), I32)
        for r, value in enumerate(values):
            w = jnp.where(subs == r, value, w)
        return w

    def packed(column):
        w = jnp.zeros((SUB, nl), I32)
        for b in range(nb):
            w = jnp.where(block == b, column[b * SUB : (b + 1) * SUB], w)
        return w

    def i_scan(w):
        d = nb
        while d < nl:
            w = w + jnp.where(lanes >= d, turn(w, d, 1), 0)
            d *= 2
        return w

    load.wait()
    total = q[0]
    for i in range(1, ni):
        total = total + q[i]
    xs[...] = total
    for i in range(ni):
        ys[pl.ds(i, 1), :] = jnp.sum(q[i], axis=0, keepdims=True)
        hy[pl.ds(i, 1), :] = q[i, 0:1, :]
    lines = jnp.where(
        sk == 0, jnp.sum(total, axis=0, keepdims=True),
        jnp.where(
            sk == 1, jnp.sum(q[0], axis=0, keepdims=True),
            jnp.where(sk == 2, total[0:1], 0),
        ),
    )
    ysv = ys[...]
    small = lane_scan(jnp.concatenate([ysv, hy[...], lines, total, q[0]], 0))[:, end]
    ends_of = jnp.broadcast_to(small[2 * ni : 2 * ni + SUB], (SUB, nl))
    whole, first_j, first_i = (ends_of[r : r + 1] for r in (0, 2, 1))
    pk[0:SUB] = stacked([
        along(small[:ni]), whole, along(ysv[:, 0:1]),
        jnp.broadcast_to(lines[0:1, 0:1], (1, nl)), in_order(small[:ni], 2),
        in_order(small[ni : 2 * ni], 3),
    ])
    pk[SUB:] = lines + stacked([
        0, 0, 0, jnp.where(within(0) | within(2), whole, 0),
        jnp.where(within(3), first_j, 0), jnp.where(within(1), first_i, 0),
    ])


    outgoing = [
        (inside(X + dx, Y + dy), functools.partial(plane_copy, n))
        for n, (dx, dy) in enumerate(plane_to)
    ] + [
        (inside(X + dx, Y + dy, Z - 1), functools.partial(level_copy, n))
        for n, (dx, dy) in enumerate(level_to)
    ]
    outgoing += [
        (inside(X + dx, Y), functools.partial(beside_copy, n)) for n, dx in enumerate(beside)
    ]
    outgoing += ups("gx", xs, xup, xss, xrs) + downs("gx", q.at[0], xdn, 0)
    outgoing += downs("gy", hy, ydn, 1) + ups("gy", ys, yup, yss, yrs)
    relays = [
        (base, (Z > 0) & (Z + base < nz) & (first_y == (base == 2)))
        for base in (1, 2) if nz > base + 1
    ]

    def burst(before=()):
        pl.semaphore_wait(barrier, awaited)
        for here, copy in [*before, *outgoing]:
            send(here, copy)
        for base, here in relays:
            @pl.when(here)
            def _(base=base):
                greet({"gz": Z - 1}, ready.at[base - 1])

    first = 2 * ni + SUB
    px[0:SUB] = j_scan(packed(small[first : first + nj]))
    px[SUB : 2 * SUB] = j_scan(packed(total[:, 0:1]))
    px[2 * SUB :] = stacked([
        in_order(small[first : first + nj], 0), in_order(small[first + nj :], 1)
    ])
    @pl.when(jnp.logical_not(first_y))
    def _():
        burst()

    deep = min(DEEP, ni)

    def scan_block(g, _):
        part = q[pl.ds(g * deep, deep)].reshape(deep * nj, nk)
        scan[pl.ds(g * deep, deep)] = lane_scan(part).reshape(deep, nj, nk)
        return 0

    lax.fori_loop(0, ni // deep, scan_block, 0)

    def columns(source, column):
        w = jnp.zeros((SUB, nl), I32)
        for i in range(ni):
            for b in range(nb):
                part = source[i, b * SUB : (b + 1) * SUB, column]
                w = jnp.where(lanes == i * nb + b, part, w)
        return i_scan(j_scan(w))

    ds[...] = columns(q, slice(0, 1))
    [(below, down_ds)] = downs("gz", ds, zdn, 2)

    @pl.when(first_y)
    def _():
        burst([(below, down_ds)])

    send(below & jnp.logical_not(first_y), down_ds)
    a0 = columns(scan, end)

    def hear(d, also):
        @pl.when((Z + d < nz) & also & (True if d > 2 else jnp.logical_not(first_y)))
        def _():
            pl.semaphore_wait(ready.at[d - 2], 1)

            if d < nz - 1:
                @pl.when(Z > 0)
                def _():
                    greet({"gz": Z - 1}, ready.at[d - 1])

    for d in range(2, nz):
        hear(d, Z > 0)

    for n, dx in enumerate(beside):
        @pl.when(inside(X - dx, Y))
        def _(n=n):
            beside_copy(n).wait_recv()

    xa = pxin[1, 0:SUB]
    for n in range(2, nx):
        xa = xa + pxin[n, 0:SUB]
    a0 = a0 + xa
    borders = pxin[0, 2 * SUB + 1 : 2 * SUB + 2]
    for n in range(1, nx):
        borders = borders + pxin[n, 2 * SUB : 2 * SUB + 1]
    z_refs = (zs, zup, zss, zrs)
    higher = ups("gz", *z_refs)
    higher_rows = ups("gz", zr, zrin, rss, rrs)
    zs[...] = a0
    hear(2, Z == 0)
    for n, (here, copy) in enumerate(higher):
        send(here & (Z > 0) if n < len(higher) - 2 else here, copy)

    def send_far():
        for d in range(3, nz):
            hear(d, Z == 0)
        for here, copy in higher[:-2]:
            send(here & (Z == 0), copy)

    up_wait("gx", xs, xup, xss, xrs)
    down_wait("gx", q.at[0], xdn, 0)
    rxv = xup[0]
    for d in range(1, nx - 1):
        rxv = rxv + xup[d]
    lx = lane_scan(jnp.concatenate([rxv, xdn[...]], 0))
    ax[...] = row_scan(lx[:nj])
    hxc[...] = row_scan(lx[nj:])

    def sweep_all():
        jrow = iota((nj, nk), 0)
        klane = iota((nj, nk), 1)
        plane = ax[...]

        def field(i, before):
            inner = before + row_scan(scan[i])
            return inner, inner + plane + by[pl.ds(i, 1), :]

        def stencil(i, low, mid, high):
            down_j = jnp.where(jrow == 0, by[pl.ds(i, 1), :], turn(mid, 1, 0))
            edge_j = jnp.where(last_y, 0, mid)
            up_j = jnp.where(jrow == nj - 1, edge_j, turn(mid, nj - 1, 0))
            down_k = jnp.where(klane == 0, 0, turn(mid, 1, 1))
            edge_k = jnp.where(last_z, 0, mid)
            up_k = jnp.where(klane == nk - 1, edge_k, turn(mid, nk - 1, 1))
            v_ref[i] = 6 * mid + (low + high) + (down_j + up_j) + (down_k + up_k)

        def sweep(i, state):
            low, mid, before = state
            inner, high = field(i + 1, before)
            stencil(i, low, mid, high)
            return mid, high, inner

        inner, mid = field(0, jnp.zeros((nj, nk), I32))
        state = (plane + tails[0:1], mid, inner)
        many = (ni - 1) // UNROLL

        def sweeps(g, state):
            for u in range(UNROLL):
                state = sweep(g * UNROLL + u, state)
            return state

        state = lax.fori_loop(0, many, sweeps, state)
        for i in range(many * UNROLL, ni - 1):
            state = sweep(i, state)
        low, mid, _ = state
        stencil(ni - 1, low, mid, jnp.where(last_x, 0, mid + hxc[...] + tails[1:2]))

    @pl.when(first_y)
    def _():
        tails[...] = jnp.zeros_like(tails)
        by[...] = jnp.zeros_like(by)
        sweep_all()
        send_far()

    for n, (dx, dy) in enumerate(plane_to):
        @pl.when(inside(X - dx, Y - dy))
        def _(n=n):
            plane_copy(n).wait_recv()

    def gather(wanted, slots):
        found = [slots(n) for n, m in enumerate(plane_to) if wanted(*m)]
        return functools.reduce(jnp.add, found) if found else jnp.zeros((SUB, nk), I32)

    kinds = (
        (lambda dx, dy: dx == 0 and dy > 0, 4), (lambda dx, dy: dx > 0 and dy > 0, SUB + 3),
        (lambda dx, dy: dx == 0 and dy < 0, 5), (lambda dx, dy: dx > 0 and dy < 0, SUB + 4),
        (lambda dx, dy: dx < 0, SUB + 5),
    )
    for wanted, r in kinds:
        at = r // SUB * SUB
        borders = borders + gather(wanted, lambda n: pkin[n, at : at + SUB])[r - at : r - at + 1]
    zr[...] = borders

    @pl.when(jnp.logical_not(first_y))
    def _():
        send_far()

    for here, copy in higher_rows:
        send(here, copy)

    up_wait("gy", ys, yup, yss, yrs)
    down_wait("gy", hy, ydn, 1)
    ryv = yup[0]
    for d in range(1, ny - 1):
        ryv = ryv + yup[d]
    rytv = stacked([
        gather(kinds[k][0], lambda n: pkin[n, SUB:])[r : r + 1] for r, k in enumerate((1, 4, 3))
    ])
    ly = lane_scan(jnp.concatenate([ryv, ydn[...], rytv], 0))
    lyl, lyh, lyt = ly[:ni], ly[ni : 2 * ni], ly[2 * ni :]
    rows_i = iota((ni, nk), 0)
    hyc[...] = row_scan(lyh + jnp.where(rows_i == 0, lyt[2:3], 0))

    @pl.when(jnp.logical_not(first_y))
    def _():
        tails[...] = lyt
        by[...] = row_scan(lyl + jnp.where(rows_i == 0, lyt[0:1], 0))
        sweep_all()

    for i in range(ni):
        beyond_j = jnp.where(sk == SUB - 1, hyc[pl.ds(i, 1), :], 0)
        v_ref[i, nj - SUB : nj, :] += jnp.where(last_y, 0, beyond_j)

    finish_sends([*outgoing, (below, down_ds)])
    for n, (dx, dy) in enumerate(level_to):
        @pl.when(inside(X - dx, Y - dy, Z + 1))
        def _(n=n):
            level_copy(n).wait_recv()

    down_wait("gz", ds, zdn, 2)
    up_wait("gz", *z_refs)
    beyond = zdn[...]
    for n, (dx, dy) in enumerate(level_to):
        r = 2 if dx == 0 else 3
        beyond = beyond + (dgin[n, r : r + 1, :] if dy else dgin[n])
    D = zup[0]
    for d in range(1, nz - 1):
        D = D + zup[d]
    prior, after = pltpu.roll(D, 1, 0), pltpu.roll(D, SUB - 1, 0)

    def raw(by):
        moved_to = lambda w, d: turn(w, d + by, 1)
        here = moved_to(D, 0)
        down_j = jnp.where(
            subs == 0, jnp.where(block == 0, 0, moved_to(prior, 1)), moved_to(prior, 0)
        )
        edge_j = jnp.where(block == nb - 1, here, moved_to(after, nl - 1))
        up_j = jnp.where(subs == SUB - 1, edge_j, moved_to(after, 0))
        return here, moved_to(D, nb), moved_to(D, nl - nb), down_j, up_j, moved_to(beyond, 0)

    raws = raw(0), raw(half)
    up_wait("gz", zr, zrin, rss, rrs)
    borders = zrin[0]
    for d in range(1, nz - 1):
        borders = borders + zrin[d]
    borders = jnp.broadcast_to(borders, D.shape)

    def pick(index):
        return jnp.take_along_axis(borders, index, 1, mode="promise_in_bounds")

    front, back = pick(block * SUB + subs), pick(nj + block * SUB + subs)
    corner_j = (subs == SUB - 1) & (block == nb - 1)

    def finals(by):
        here, down_i, up_i, down_j, up_j, past = raws[by // half]
        at = lax.rem(lanes + (nl - by), nl)
        g = at // nb
        low = pick(starts[2] + g)
        here = here + low
        down_i = jnp.where(at < nb, front, down_i + pick(starts[2] + jnp.maximum(g - 1, 0)))
        edge_i = jnp.where(last_x, 0, here + back)
        next_low = pick(starts[2] + jnp.minimum(g + 1, ni - 1))
        up_i = jnp.where(at >= nl - nb, edge_i, up_i + next_low)
        edge_j = jnp.where(last_y, 0, here + pick(starts[3] + g))
        up_j = jnp.where(corner_j, edge_j, up_j + low)
        E = 8 * here + (down_i + up_i) + (down_j + low + up_j)
        return E, E + jnp.where(last_z, -here, past)

    E, EH = finals(0)
    E_half, EH_half = finals(half)
    eh_ref[0:SUB] = jnp.where(lanes < half, E, EH_half)
    eh_ref[SUB : 2 * SUB] = jnp.where(lanes < half, E_half, EH)

    finish_sends([*higher, *higher_rows])


def messages(nx, ny):
    plane = [(dx, -1) for dx in range(nx)] + [
        (dx, dy) for dy in range(ny - 1, 0, -1) for dx in range(-1, nx)
    ]
    level = [(dx, dy) for dy in range(ny - 1, -1, -1) for dx in range(nx) if dx or dy]
    return plane, level


def finish(step_ref, v_ref, eh_ref, out_hbm, out, sems):
    ni, nj, nk = out.shape
    nb = nj // SUB
    scale = step_ref[0] * (1.0 / 12.0)
    half = ni * nb // 2
    base = jnp.where(iota((SUB, nk), 1) == nk - 1, half, 0)
    halves = eh_ref[0:SUB], eh_ref[SUB : 2 * SUB]
    steps = sems.shape[0] // 2
    depth = ni // 2 // steps
    turned = [[turn(w, half * 2 - c, 1) for c in range(TURNS)] for w in halves]
    copies = []
    for p in range(steps):
        for i in range(p * depth, (p + 1) * depth):
            for b in range(nb):
                v = i * nb + b
                c = v % TURNS
                rows = slice(b * SUB, (b + 1) * SUB)
                for at, source in ((i, turned[0][c]), (i + ni // 2, turned[1][c])):
                    carry = jnp.take_along_axis(
                        source, base + (v - c), 1, mode="promise_in_bounds"
                    )
                    out[at, rows, :] = (v_ref[at, rows, :] + carry).astype(F32) * scale
        for h in range(2):
            part = pl.ds(h * (ni // 2) + p * depth, depth)
            copy = pltpu.make_async_copy(out.at[part], out_hbm.at[part], sems.at[2 * p + h])
            copy.start()
            copies.append(copy)
    for copy in copies:
        copy.wait()


def solution(mesh):
    sizes = tuple(mesh.shape[a] for a in ("gx", "gy", "gz"))
    nx, ny, nz = sizes

    def on_device(quant_codes, error_step):
        ni, nj, nk = quant_codes.shape
        nl = ni * nj // SUB
        vm = lambda *shape: pltpu.VMEM(shape, I32)
        dma = lambda n: pltpu.SemaphoreType.DMA((n,))
        plane_to, level_to = messages(nx, ny)
        np_, ng = len(plane_to), len(level_to)
        scratch = [
            vm(ni, nj, nk), vm(ni, nj, nk),
            vm(nj, nk), vm(nx - 1, nj, nk), vm(nj, nk),
            vm(ni, nk), vm(ny - 1, ni, nk), vm(ni, nk), vm(ni, nk),
            vm(2 * SUB, nl), vm(np_, 2 * SUB, nl), vm(3 * SUB, nl), vm(nx, 3 * SUB, nl),
            vm(ng, SUB, nl),
            vm(SUB, nl), vm(nz - 1, SUB, nl), vm(1, nl), vm(nz - 1, 1, nl),
            vm(SUB, nl), vm(SUB, nl),
            vm(nj, nk), vm(nj, nk), vm(ni, nk), vm(ni, nk), vm(SUB, nk),
        ]
        semaphores = [
            pltpu.SemaphoreType.DMA,
            dma(nx - 1), dma(nx - 1), dma(ny - 1), dma(ny - 1),
            dma(np_), dma(np_), dma(nx), dma(nx), dma(ng), dma(ng), *[dma(nz - 1)] * 4,
            dma(3), dma(3),
            pltpu.SemaphoreType.REGULAR((max(nz - 2, 1),)),
        ]

        def scoped(*refs):
            def body(*sems):
                exchange(sizes, *refs, *sems)

            pl.run_scoped(body, *semaphores)

        any_space = pl.BlockSpec(memory_space=pl.ANY)
        hbm = pl.BlockSpec(memory_space=pltpu.HBM)
        vmem = pl.BlockSpec(memory_space=pltpu.VMEM)
        v, eh = pl.pallas_call(
            scoped,
            out_shape=(
                jax.ShapeDtypeStruct((ni, nj, nk), I32),
                jax.ShapeDtypeStruct((2 * SUB, nl), I32),
            ),
            in_specs=[hbm],
            out_specs=(vmem, vmem),
            scratch_shapes=scratch,
            compiler_params=pltpu.CompilerParams(
                collective_id=0, has_side_effects=True, vmem_limit_bytes=GRANT
            ),
            name="exchange",
        )(pltpu.with_memory_space_constraint(quant_codes, pltpu.HBM))
        def finish_scoped(*refs):
            pl.run_scoped(functools.partial(finish, *refs), dma(8))

        return pl.pallas_call(
            finish_scoped,
            out_shape=jax.ShapeDtypeStruct((ni, nj, nk), F32),
            in_specs=[pl.BlockSpec(memory_space=pltpu.SMEM), vmem, vmem],
            out_specs=any_space,
            scratch_shapes=[pltpu.VMEM((ni, nj, nk), F32)],
            compiler_params=pltpu.CompilerParams(vmem_limit_bytes=16 * 2**20),
            name="finish",
        )(error_step, v, eh)

    return jax.shard_map(
        on_device, mesh=mesh, in_specs=(P("gx", "gy", "gz"), P()),
        out_specs=P("gx", "gy", "gz"), check_vma=False,
    )
```

```python
import functools

import jax
import jax.numpy as jnp
from jax import lax
from jax.experimental import pallas as pl
from jax.experimental.pallas import tpu as pltpu
from jax.sharding import PartitionSpec as P

MESH = pl.DeviceIdType.MESH
I32 = jnp.int32
F32 = jnp.float32
SUB = 8
GRANT = 16 * 2**20
UNROLL = 4
DEEP = 16
TURNS = 8


def iota(shape, dim):
    return lax.broadcasted_iota(I32, shape, dim)


def turn(x, by, dim):
    n = x.shape[dim]
    by = by % n
    if by == 0:
        return x
    if dim == 1 and n % 128 != 0:
        return jnp.concatenate([x[:, n - by :], x[:, : n - by]], 1)
    return pltpu.roll(x, by, dim)


def lane_scan(x):
    n = x.shape[1]
    tri = (iota((n, n), 0) <= iota((n, n), 1)).astype(F32)
    one, big = tri.astype(jnp.bfloat16), (tri * 256.0).astype(jnp.bfloat16)

    def times(part, m):
        return jnp.dot(part.astype(F32).astype(jnp.bfloat16), m, preferred_element_type=F32)

    low = times(x & 255, one) + times((x >> 8) & 255, big)
    high = times((x >> 16) & 255, one) + times(x >> 24, big)
    return low.astype(I32) + (high.astype(I32) << 16)


def row_scan(x):
    rows, n = x.shape
    s = iota((SUB, n), 0)
    out, carry = [], None
    for b in range(rows // SUB):
        v = x[b * SUB : (b + 1) * SUB]
        for d in (1, 2, 4):
            v = v + jnp.where(s >= d, pltpu.roll(v, d, 0), 0)
        if carry is not None:
            v = v + carry
        carry = jnp.broadcast_to(v[SUB - 1 : SUB], (SUB, n))
        out.append(v)
    return jnp.concatenate(out, 0) if len(out) > 1 else out[0]


def exchange(
    mesh_sizes, q_hbm, v_ref, eh_ref,
    q, scan, xs, xup, xdn, ys, yup, hy, ydn, pr, prin, pk, pkin, px, pxin, dgin,
    zs, zup, zr, zrin, ds, zdn, ax, hxc, by, hyc, tails,
    load_sem, xss, xrs, yss, yrs, pss, prs, ass, ars, gss, grs, zss, zrs, rss, rrs, dss, drs, ready,
):
    nx, ny, nz = mesh_sizes
    ni, nj, nk = q.shape
    nb = nj // SUB
    nl = ni * nb
    X, Y, Z = (lax.axis_index(a) for a in ("gx", "gy", "gz"))
    place = {"gx": X, "gy": Y, "gz": Z}
    size = {"gx": nx, "gy": ny, "gz": nz}
    last_x, last_y, last_z = X == nx - 1, Y == ny - 1, Z == nz - 1
    plane_to, level_to = messages(nx, ny)
    beside = [-1, *range(1, nx)]

    load = pltpu.make_async_copy(q_hbm, q, load_sem)
    load.start()
    barrier = pltpu.get_barrier_semaphore()

    def greet(to, sem):
        pl.semaphore_signal(sem, inc=1, device_id=to, device_id_type=MESH)

    def inside(x, y, z=0):
        ok = (x >= 0) & (x < nx) & (y >= 0) & (y < ny)
        return ok if isinstance(z, int) else ok & (z >= 0) & (z < nz)

    def greet_plane(dx, dy):
        greet({"gx": lax.rem(X + dx, nx), "gy": lax.rem(Y + dy, ny)}, barrier)

    for dy in range(1, ny):
        greet_plane(0, dy)
    first_y = Y == 0
    for d in (-2, -1, 1):
        @pl.when((Z + d >= 0) & (Z + d < nz) & (first_y if d == -2 else True))
        def _(d=d):
            greet({"gz": Z + d}, barrier)

    for dx in range(1, nx):
        for dy in range(ny):
            greet_plane(dx, dy)

    for dx, dy in level_to:
        @pl.when(inside(X - dx, Y - dy, Z + 1))
        def _(dx=dx, dy=dy):
            greet({"gx": X - dx, "gy": Y - dy, "gz": Z + 1}, barrier)

    near = sum(((Z + d >= 0) & (Z + d < nz)).astype(I32) for d in (-1, 1))
    near = near + (first_y & (Z + 2 < nz)).astype(I32)
    above = jnp.where(Z > 0, (nx - X) * (ny - Y) - 1, 0)
    awaited = nx * ny - 1 + near + above

    def clear(here, slot):
        @pl.when(here)
        def _():
            slot[...] = jnp.zeros(slot.shape, I32)

    for n, (dx, dy) in enumerate(plane_to):
        clear(jnp.logical_not(inside(X - dx, Y - dy)), pkin.at[n])
    for n, dx in enumerate(beside):
        clear(jnp.logical_not(inside(X - dx, Y)), pxin.at[n])
    for n, (dx, dy) in enumerate(level_to):
        clear(jnp.logical_not(inside(X - dx, Y - dy, Z + 1)), dgin.at[n])
    for axis, slots, beyond in (("gx", xup, xdn), ("gy", yup, ydn), ("gz", zup, zdn), ("gz", zrin, None), ("gy", None, prin)):
        for d in range(1, size[axis]) if slots is not None else ():
            clear(place[axis] < d, slots.at[d - 1])
        if beyond is not None:
            clear(place[axis] == size[axis] - 1, beyond)

    def send(here, copy):
        @pl.when(here)
        def _():
            copy().start()

    def finish_sends(started):
        for here, copy in started:
            @pl.when(here)
            def _(copy=copy):
                copy().wait_send()

    def up_copy(axis, src, slots, ssem, rsem, d):
        return pltpu.make_async_remote_copy(
            src_ref=src, dst_ref=slots.at[d - 1], send_sem=ssem.at[d - 1],
            recv_sem=rsem.at[d - 1], device_id={axis: place[axis] + d},
            device_id_type=MESH,
        )

    def ups(axis, *refs):
        return [
            (place[axis] + d < size[axis], functools.partial(up_copy, axis, *refs, d))
            for d in range(size[axis] - 1, 0, -1)
        ]

    def up_wait(axis, *refs):
        for d in range(1, size[axis]):
            @pl.when(place[axis] >= d)
            def _(d=d):
                up_copy(axis, *refs, d).wait_recv()

    def down_copy(axis, src, dst, n):
        return pltpu.make_async_remote_copy(
            src_ref=src, dst_ref=dst, send_sem=dss.at[n], recv_sem=drs.at[n],
            device_id={axis: place[axis] - 1}, device_id_type=MESH,
        )

    def downs(axis, src, dst, n):
        return [(place[axis] > 0, functools.partial(down_copy, axis, src, dst, n))]

    def down_wait(axis, src, dst, n):
        @pl.when(place[axis] < size[axis] - 1)
        def _():
            down_copy(axis, src, dst, n).wait_recv()

    def plane_copy(n):
        return pltpu.make_async_remote_copy(
            src_ref=pk if plane_to[n][0] else pk.at[0:SUB],
            dst_ref=pkin.at[n] if plane_to[n][0] else pkin.at[n, 0:SUB],
            send_sem=pss.at[n], recv_sem=prs.at[n],
            device_id={"gx": X + plane_to[n][0], "gy": Y + plane_to[n][1]},
            device_id_type=MESH,
        )

    def beside_copy(n):
        return pltpu.make_async_remote_copy(
            src_ref=px, dst_ref=pxin.at[n], send_sem=ass.at[n], recv_sem=ars.at[n],
            device_id={"gx": X + beside[n]}, device_id_type=MESH,
        )

    def level_copy(n):
        return pltpu.make_async_remote_copy(
            src_ref=pk.at[0:SUB] if level_to[n][1] else px.at[SUB : 2 * SUB],
            dst_ref=dgin.at[n], send_sem=gss.at[n],
            recv_sem=grs.at[n], device_id_type=MESH,
            device_id={"gx": X + level_to[n][0], "gy": Y + level_to[n][1], "gz": Z - 1},
        )

    lanes = iota((SUB, nl), 1)
    subs = iota((SUB, nl), 0)
    sk = iota((SUB, nk), 0)
    block = lax.rem(lanes, nb)
    half = nl // 2
    starts = (0, nj, 2 * nj, 2 * nj + ni, 2 * (nj + ni))
    lane = iota((1, nl), 1)

    def within(k):
        return (lane >= starts[k]) & (lane < starts[k + 1])

    def in_order(column, k):
        n = column.shape[0]
        at = iota((n, nl), 1) - starts[k]
        reached = (at >= iota((n, nl), 0)) & (at < n)
        return jnp.sum(jnp.where(reached, column, 0), axis=0, keepdims=True)
    end = slice(nk - 1, nk)
    upto = (iota((ni, nl), 1) // nb) >= iota((ni, nl), 0)

    def along(column):
        return jnp.sum(jnp.where(upto, column, 0), axis=0, keepdims=True)

    def j_scan(w):
        for d in (1, 2, 4):
            w = w + jnp.where(subs >= d, pltpu.roll(w, d, 0), 0)
        whole = jnp.broadcast_to(w[SUB - 1 : SUB], w.shape)
        for d in range(1, nb):
            w = w + jnp.where(block >= d, turn(whole, d, 1), 0)
        return w

    def stacked(values):
        w = jnp.zeros((SUB, nl), I32)
        for r, value in enumerate(values):
            w = jnp.where(subs == r, value, w)
        return w

    def packed(column):
        w = jnp.zeros((SUB, nl), I32)
        for b in range(nb):
            w = jnp.where(block == b, column[b * SUB : (b + 1) * SUB], w)
        return w

    def i_scan(w):
        d = nb
        while d < nl:
            w = w + jnp.where(lanes >= d, turn(w, d, 1), 0)
            d *= 2
        return w

    load.wait()
    total = q[0]
    for i in range(1, ni):
        total = total + q[i]
    xs[...] = total
    for i in range(ni):
        ys[pl.ds(i, 1), :] = jnp.sum(q[i], axis=0, keepdims=True)
        hy[pl.ds(i, 1), :] = q[i, 0:1, :]
    lines = jnp.where(
        sk == 0, jnp.sum(total, axis=0, keepdims=True),
        jnp.where(
            sk == 1, jnp.sum(q[0], axis=0, keepdims=True),
            jnp.where(sk == 2, total[0:1], 0),
        ),
    )
    ysv = ys[...]
    small = lane_scan(jnp.concatenate([ysv, hy[...], lines, total, q[0]], 0))[:, end]
    ends_of = jnp.broadcast_to(small[2 * ni : 2 * ni + SUB], (SUB, nl))
    whole, first_j, first_i = (ends_of[r : r + 1] for r in (0, 2, 1))
    pk[0:SUB] = stacked([
        along(small[:ni]), whole, along(ysv[:, 0:1]),
        jnp.broadcast_to(lines[0:1, 0:1], (1, nl)), in_order(small[:ni], 2),
    ])
    pr[...] = in_order(small[ni : 2 * ni], 3)
    pk[SUB:] = lines + stacked([
        0, 0, 0, jnp.where(within(0) | within(2), whole, 0),
        jnp.where(within(3), first_j, 0), jnp.where(within(1), first_i, 0),
    ])


    outgoing = downs("gy", pr, prin, 3) + [
        (inside(X + dx, Y + dy), functools.partial(plane_copy, n))
        for n, (dx, dy) in enumerate(plane_to)
    ] + [
        (inside(X + dx, Y + dy, Z - 1), functools.partial(level_copy, n))
        for n, (dx, dy) in enumerate(level_to)
    ]
    outgoing += [
        (inside(X + dx, Y), functools.partial(beside_copy, n)) for n, dx in enumerate(beside)
    ]
    outgoing += ups("gx", xs, xup, xss, xrs) + downs("gx", q.at[0], xdn, 0)
    outgoing += downs("gy", hy, ydn, 1) + ups("gy", ys, yup, yss, yrs)
    relays = [
        (base, (Z > 0) & (Z + base < nz) & (first_y == (base == 2)))
        for base in (1, 2) if nz > base + 1
    ]

    def burst(before=()):
        pl.semaphore_wait(barrier, awaited)
        for here, copy in [*before, *outgoing]:
            send(here, copy)
        for base, here in relays:
            @pl.when(here)
            def _(base=base):
                greet({"gz": Z - 1}, ready.at[base - 1])

    first = 2 * ni + SUB
    px[0:SUB] = j_scan(packed(small[first : first + nj]))
    px[SUB : 2 * SUB] = j_scan(packed(total[:, 0:1]))
    px[2 * SUB :] = stacked([
        in_order(small[first : first + nj], 0), in_order(small[first + nj :], 1)
    ])
    @pl.when(jnp.logical_not(first_y))
    def _():
        burst()

    deep = min(DEEP, ni)

    def scan_block(g, _):
        part = q[pl.ds(g * deep, deep)].reshape(deep * nj, nk)
        scan[pl.ds(g * deep, deep)] = lane_scan(part).reshape(deep, nj, nk)
        return 0

    lax.fori_loop(0, ni // deep, scan_block, 0)

    def columns(source, column):
        w = jnp.zeros((SUB, nl), I32)
        for i in range(ni):
            for b in range(nb):
                part = source[i, b * SUB : (b + 1) * SUB, column]
                w = jnp.where(lanes == i * nb + b, part, w)
        return i_scan(j_scan(w))

    ds[...] = columns(q, slice(0, 1))
    [(below, down_ds)] = downs("gz", ds, zdn, 2)

    @pl.when(first_y)
    def _():
        burst([(below, down_ds)])

    send(below & jnp.logical_not(first_y), down_ds)
    a0 = columns(scan, end)

    def hear(d, also):
        @pl.when((Z + d < nz) & also & (True if d > 2 else jnp.logical_not(first_y)))
        def _():
            pl.semaphore_wait(ready.at[d - 2], 1)

            if d < nz - 1:
                @pl.when(Z > 0)
                def _():
                    greet({"gz": Z - 1}, ready.at[d - 1])

    for d in range(2, nz):
        hear(d, Z > 0)

    for n, dx in enumerate(beside):
        @pl.when(inside(X - dx, Y))
        def _(n=n):
            beside_copy(n).wait_recv()

    xa = pxin[1, 0:SUB]
    for n in range(2, nx):
        xa = xa + pxin[n, 0:SUB]
    a0 = a0 + xa
    borders = pxin[0, 2 * SUB + 1 : 2 * SUB + 2]
    for n in range(1, nx):
        borders = borders + pxin[n, 2 * SUB : 2 * SUB + 1]
    z_refs = (zs, zup, zss, zrs)
    higher = ups("gz", *z_refs)
    higher_rows = ups("gz", zr, zrin, rss, rrs)
    zs[...] = a0
    hear(2, Z == 0)
    for n, (here, copy) in enumerate(higher):
        send(here & (Z > 0) if n < len(higher) - 2 else here, copy)

    def send_far():
        for d in range(3, nz):
            hear(d, Z == 0)
        for here, copy in higher[:-2]:
            send(here & (Z == 0), copy)

    up_wait("gx", xs, xup, xss, xrs)
    down_wait("gx", q.at[0], xdn, 0)
    rxv = xup[0]
    for d in range(1, nx - 1):
        rxv = rxv + xup[d]
    lx = lane_scan(jnp.concatenate([rxv, xdn[...]], 0))
    ax[...] = row_scan(lx[:nj])
    hxc[...] = row_scan(lx[nj:])

    def sweep_all():
        jrow = iota((nj, nk), 0)
        klane = iota((nj, nk), 1)
        plane = ax[...]

        def field(i, before):
            inner = before + row_scan(scan[i])
            return inner, inner + plane + by[pl.ds(i, 1), :]

        def stencil(i, low, mid, high):
            down_j = jnp.where(jrow == 0, by[pl.ds(i, 1), :], turn(mid, 1, 0))
            edge_j = jnp.where(last_y, 0, mid)
            up_j = jnp.where(jrow == nj - 1, edge_j, turn(mid, nj - 1, 0))
            down_k = jnp.where(klane == 0, 0, turn(mid, 1, 1))
            edge_k = jnp.where(last_z, 0, mid)
            up_k = jnp.where(klane == nk - 1, edge_k, turn(mid, nk - 1, 1))
            v_ref[i] = 6 * mid + (low + high) + (down_j + up_j) + (down_k + up_k)

        def sweep(i, state):
            low, mid, before = state
            inner, high = field(i + 1, before)
            stencil(i, low, mid, high)
            return mid, high, inner

        inner, mid = field(0, jnp.zeros((nj, nk), I32))
        state = (plane + tails[0:1], mid, inner)
        many = (ni - 1) // UNROLL

        def sweeps(g, state):
            for u in range(UNROLL):
                state = sweep(g * UNROLL + u, state)
            return state

        state = lax.fori_loop(0, many, sweeps, state)
        for i in range(many * UNROLL, ni - 1):
            state = sweep(i, state)
        low, mid, _ = state
        stencil(ni - 1, low, mid, jnp.where(last_x, 0, mid + hxc[...] + tails[1:2]))

    @pl.when(first_y)
    def _():
        tails[...] = jnp.zeros_like(tails)
        by[...] = jnp.zeros_like(by)
        sweep_all()
        send_far()

    for n, (dx, dy) in enumerate(plane_to):
        @pl.when(inside(X - dx, Y - dy))
        def _(n=n):
            plane_copy(n).wait_recv()

    down_wait("gy", pr, prin, 3)
    borders = borders + prin[...]

    def gather(wanted, slots):
        found = [slots(n) for n, m in enumerate(plane_to) if wanted(*m)]
        return functools.reduce(jnp.add, found) if found else jnp.zeros((SUB, nk), I32)

    kinds = (
        (lambda dx, dy: dx == 0 and dy > 0, 4), (lambda dx, dy: dx > 0 and dy > 0, SUB + 3),
        (lambda dx, dy: dx > 0 and dy < 0, SUB + 4),
        (lambda dx, dy: dx < 0, SUB + 5),
    )
    for wanted, r in kinds:
        at = r // SUB * SUB
        borders = borders + gather(wanted, lambda n: pkin[n, at : at + SUB])[r - at : r - at + 1]
    zr[...] = borders

    @pl.when(jnp.logical_not(first_y))
    def _():
        send_far()

    for here, copy in higher_rows:
        send(here, copy)

    up_wait("gy", ys, yup, yss, yrs)
    down_wait("gy", hy, ydn, 1)
    ryv = yup[0]
    for d in range(1, ny - 1):
        ryv = ryv + yup[d]
    rytv = stacked([
        gather(kinds[k][0], lambda n: pkin[n, SUB:])[r : r + 1] for r, k in enumerate((1, 3, 2))
    ])
    ly = lane_scan(jnp.concatenate([ryv, ydn[...], rytv], 0))
    lyl, lyh, lyt = ly[:ni], ly[ni : 2 * ni], ly[2 * ni :]
    rows_i = iota((ni, nk), 0)
    hyc[...] = row_scan(lyh + jnp.where(rows_i == 0, lyt[2:3], 0))

    @pl.when(jnp.logical_not(first_y))
    def _():
        tails[...] = lyt
        by[...] = row_scan(lyl + jnp.where(rows_i == 0, lyt[0:1], 0))
        sweep_all()

    for i in range(ni):
        beyond_j = jnp.where(sk == SUB - 1, hyc[pl.ds(i, 1), :], 0)
        v_ref[i, nj - SUB : nj, :] += jnp.where(last_y, 0, beyond_j)

    finish_sends([*outgoing, (below, down_ds)])
    up_wait("gz", *z_refs)
    D = zup[0]
    for d in range(1, nz - 1):
        D = D + zup[d]
    prior, after = pltpu.roll(D, 1, 0), pltpu.roll(D, SUB - 1, 0)

    def raw(by):
        moved_to = lambda w, d: turn(w, d + by, 1)
        here = moved_to(D, 0)
        down_j = jnp.where(
            subs == 0, jnp.where(block == 0, 0, moved_to(prior, 1)), moved_to(prior, 0)
        )
        edge_j = jnp.where(block == nb - 1, here, moved_to(after, nl - 1))
        up_j = jnp.where(subs == SUB - 1, edge_j, moved_to(after, 0))
        return here, moved_to(D, nb), moved_to(D, nl - nb), down_j, up_j

    raws = raw(0), raw(half)
    up_wait("gz", zr, zrin, rss, rrs)
    borders = zrin[0]
    for d in range(1, nz - 1):
        borders = borders + zrin[d]
    borders = jnp.broadcast_to(borders, D.shape)

    def pick(index):
        return jnp.take_along_axis(borders, index, 1, mode="promise_in_bounds")

    front, back = pick(block * SUB + subs), pick(nj + block * SUB + subs)
    corner_j = (subs == SUB - 1) & (block == nb - 1)

    def finals(by):
        here, down_i, up_i, down_j, up_j = raws[by // half]
        at = lax.rem(lanes + (nl - by), nl)
        g = at // nb
        low = pick(starts[2] + g)
        here = here + low
        down_i = jnp.where(at < nb, front, down_i + pick(starts[2] + jnp.maximum(g - 1, 0)))
        edge_i = jnp.where(last_x, 0, here + back)
        next_low = pick(starts[2] + jnp.minimum(g + 1, ni - 1))
        up_i = jnp.where(at >= nl - nb, edge_i, up_i + next_low)
        edge_j = jnp.where(last_y, 0, here + pick(starts[3] + g))
        up_j = jnp.where(corner_j, edge_j, up_j + low)
        E = 8 * here + (down_i + up_i) + (down_j + low + up_j)
        return E, here

    (E, here), (E_half, here_half) = finals(0), finals(half)
    for n, (dx, dy) in enumerate(level_to):
        @pl.when(inside(X - dx, Y - dy, Z + 1))
        def _(n=n):
            level_copy(n).wait_recv()

    down_wait("gz", ds, zdn, 2)
    beyond = zdn[...]
    for n, (dx, dy) in enumerate(level_to):
        r = 2 if dx == 0 else 3
        beyond = beyond + (dgin[n, r : r + 1, :] if dy else dgin[n])
    EH = E + jnp.where(last_z, -here, beyond)
    EH_half = E_half + jnp.where(last_z, -here_half, turn(beyond, half, 1))
    eh_ref[0:SUB] = jnp.where(lanes < half, E, EH_half)
    eh_ref[SUB : 2 * SUB] = jnp.where(lanes < half, E_half, EH)

    finish_sends([*higher, *higher_rows])


def messages(nx, ny):
    plane = [(dx, -1) for dx in range(1, nx)] + [
        (dx, dy) for dy in range(ny - 1, 0, -1) for dx in range(-1, nx)
    ]
    level = [(dx, dy) for dy in range(ny - 1, -1, -1) for dx in range(nx) if dx or dy]
    return plane, level


def finish(step_ref, v_ref, eh_ref, out_hbm, out, sems):
    ni, nj, nk = out.shape
    nb = nj // SUB
    scale = step_ref[0] * (1.0 / 12.0)
    half = ni * nb // 2
    base = jnp.where(iota((SUB, nk), 1) == nk - 1, half, 0)
    halves = eh_ref[0:SUB], eh_ref[SUB : 2 * SUB]
    steps = sems.shape[0] // 2
    depth = ni // 2 // steps
    turned = [[turn(w, half * 2 - c, 1) for c in range(TURNS)] for w in halves]
    copies = []
    for p in range(steps):
        for i in range(p * depth, (p + 1) * depth):
            for b in range(nb):
                v = i * nb + b
                c = v % TURNS
                rows = slice(b * SUB, (b + 1) * SUB)
                for at, source in ((i, turned[0][c]), (i + ni // 2, turned[1][c])):
                    carry = jnp.take_along_axis(
                        source, base + (v - c), 1, mode="promise_in_bounds"
                    )
                    out[at, rows, :] = (v_ref[at, rows, :] + carry).astype(F32) * scale
        for h in range(2):
            part = pl.ds(h * (ni // 2) + p * depth, depth)
            copy = pltpu.make_async_copy(out.at[part], out_hbm.at[part], sems.at[2 * p + h])
            copy.start()
            copies.append(copy)
    for copy in copies:
        copy.wait()


def solution(mesh):
    sizes = tuple(mesh.shape[a] for a in ("gx", "gy", "gz"))
    nx, ny, nz = sizes

    def on_device(quant_codes, error_step):
        ni, nj, nk = quant_codes.shape
        nl = ni * nj // SUB
        vm = lambda *shape: pltpu.VMEM(shape, I32)
        dma = lambda n: pltpu.SemaphoreType.DMA((n,))
        plane_to, level_to = messages(nx, ny)
        np_, ng = len(plane_to), len(level_to)
        scratch = [
            vm(ni, nj, nk), vm(ni, nj, nk),
            vm(nj, nk), vm(nx - 1, nj, nk), vm(nj, nk),
            vm(ni, nk), vm(ny - 1, ni, nk), vm(ni, nk), vm(ni, nk),
            vm(1, nl), vm(1, nl), vm(2 * SUB, nl), vm(np_, 2 * SUB, nl), vm(3 * SUB, nl), vm(nx, 3 * SUB, nl),
            vm(ng, SUB, nl),
            vm(SUB, nl), vm(nz - 1, SUB, nl), vm(1, nl), vm(nz - 1, 1, nl),
            vm(SUB, nl), vm(SUB, nl),
            vm(nj, nk), vm(nj, nk), vm(ni, nk), vm(ni, nk), vm(SUB, nk),
        ]
        semaphores = [
            pltpu.SemaphoreType.DMA,
            dma(nx - 1), dma(nx - 1), dma(ny - 1), dma(ny - 1),
            dma(np_), dma(np_), dma(nx), dma(nx), dma(ng), dma(ng), *[dma(nz - 1)] * 4,
            dma(4), dma(4),
            pltpu.SemaphoreType.REGULAR((max(nz - 2, 1),)),
        ]

        def scoped(*refs):
            def body(*sems):
                exchange(sizes, *refs, *sems)

            pl.run_scoped(body, *semaphores)

        any_space = pl.BlockSpec(memory_space=pl.ANY)
        hbm = pl.BlockSpec(memory_space=pltpu.HBM)
        vmem = pl.BlockSpec(memory_space=pltpu.VMEM)
        v, eh = pl.pallas_call(
            scoped,
            out_shape=(
                jax.ShapeDtypeStruct((ni, nj, nk), I32),
                jax.ShapeDtypeStruct((2 * SUB, nl), I32),
            ),
            in_specs=[hbm],
            out_specs=(vmem, vmem),
            scratch_shapes=scratch,
            compiler_params=pltpu.CompilerParams(
                collective_id=0, has_side_effects=True, vmem_limit_bytes=GRANT
            ),
            name="exchange",
        )(pltpu.with_memory_space_constraint(quant_codes, pltpu.HBM))
        def finish_scoped(*refs):
            pl.run_scoped(functools.partial(finish, *refs), dma(8))

        return pl.pallas_call(
            finish_scoped,
            out_shape=jax.ShapeDtypeStruct((ni, nj, nk), F32),
            in_specs=[pl.BlockSpec(memory_space=pltpu.SMEM), vmem, vmem],
            out_specs=any_space,
            scratch_shapes=[pltpu.VMEM((ni, nj, nk), F32)],
            compiler_params=pltpu.CompilerParams(vmem_limit_bytes=16 * 2**20),
            name="finish",
        )(error_step, v, eh)

    return jax.shard_map(
        on_device, mesh=mesh, in_specs=(P("gx", "gy", "gz"), P()),
        out_specs=P("gx", "gy", "gz"), check_vma=False,
    )
```
